32 devices in a mesh: groups: 2 (over y), res: 8 (over z, x), seq: 2 (over core).
Axes of the slice: x: 2, y: 2, z: 4, core: 2. Of those that a mesh axis runs over, the one named last changes fastest.
Arguments:
- alignment: bfloat16 [128, 32, 256], P(('groups', 'seq'), 'res'), parts along dimension 0, may hold values from -6 to 6
- ln_gain: float32 [256], replicated, may hold values from 0.1 to 1.9
- proj_left: bfloat16 [256, 32], replicated, may hold values from -0.375 to 0.375
- proj_right: bfloat16 [256, 32], replicated, may hold values from -0.375 to 0.375
- out_weight: bfloat16 [1024, 128], replicated, may hold values from -4 to 4
- out_bias: float32 [128], replicated, may hold values from -3 to 3
Outputs:
- pair_update: bfloat16 [64, 32, 128], P(('groups', 'res'), 'seq'), parts along dimension 0
The draws below stay inside these ranges and needn't reach their ends.
There are 2 independent parts, one for each index of `groups`. The reference program is written for one: setup_inputs(seed, part) draws one part's arguments, and reference() takes and returns one part's arrays. A program takes and returns all parts, laid end to end along the dimension named above; an argument that names none is the same for every part. Nothing has to cross between parts.
All inputs are finite; a program needn't handle non-finite values.
Results may differ from the reference program's by a relative error of at most 0.0095.
Values may be sent and summed in bfloat16 or wider, within the bound.
A program may use at most 64 MiB of HBM per device.

```python
import math
import jax
import jax.numpy as jnp
from jax import lax

CM = 256
CH = 32
CZ = 128
SEQS = 64
RES = 32


def steps_of(rng, dims, cuts, smallest, largest):
    loudness, own = 1.0, jax.random.fold_in(rng, 6)
    for axis_at, blocks in cuts:
        draws = jnp.exp(jax.random.uniform(jax.random.fold_in(own, axis_at), (blocks,), jnp.float32, smallest / len(cuts), largest / len(cuts)))
        loudness = loudness * jnp.repeat(draws, dims[axis_at] // blocks).reshape([-1 if axis == axis_at else 1 for axis in range(len(dims))])
    return loudness


def normal_values(key, shape, width, most, shards=(), kind=jnp.bfloat16):
    values = width * jax.random.normal(key, shape, jnp.float32)
    if shards:
        values = values * steps_of(key, shape, shards, -0.22, 0.18)
    return jnp.clip(values, -most, most).astype(kind)


def setup_inputs(seed: int = 0, part: int = 0) -> dict:
    splits = jax.random.split(jax.random.key(seed), 7)
    part_keys = jax.random.split(jax.random.fold_in(splits[6], part), 7)
    return {
        "alignment": normal_values(part_keys[0], (SEQS, RES, CM), 1.0, 6.0, ((0, 2), (1, 8))),
        "ln_gain": jnp.clip(1.0 + 0.18 * jax.random.normal(splits[1], (CM,), jnp.float32), 0.1, 1.9),
        "proj_left": normal_values(splits[2], (CM, CH), CM ** -0.5, 0.375),
        "proj_right": normal_values(splits[3], (CM, CH), CM ** -0.5, 0.375),
        "out_weight": normal_values(splits[4], (CH * CH, CZ), (SEQS ** 0.5 / CH), 4.0),
        "out_bias": normal_values(splits[5], (CZ,), 0.5, 3.0, (), jnp.float32),
    }


def normalize(alignment, ln_gain):
    values = alignment.astype(jnp.float32)
    centred = values - lax.optimization_barrier(jnp.mean(values, axis=-1, keepdims=True))
    variance = lax.optimization_barrier(jnp.mean(centred * centred, axis=-1, keepdims=True))
    return (centred * lax.rsqrt(variance + 1e-05) * ln_gain).astype(jnp.bfloat16)

def project_in(normed, weight):
    flat_rows = normed.reshape(-1, normed.shape[2])
    projected = jnp.dot(flat_rows, weight, preferred_element_type=jnp.float32).astype(jnp.bfloat16)
    return projected.reshape(normed.shape[0], normed.shape[1], weight.shape[1])

def reference(alignment, ln_gain, proj_left, proj_right, out_weight, out_bias):
    normed = normalize(alignment, ln_gain)
    left_side = project_in(normed, proj_left)
    right_side = project_in(normed, proj_right)
    right_flat = right_side.reshape(SEQS, RES * CH)
    weight_full = out_weight.astype(jnp.float32)
    block_width = math.gcd(RES, 8)

    def row_block(position):
        picked = lax.dynamic_slice_in_dim(left_side, position * block_width, block_width, 1)
        picked = picked.reshape(SEQS, block_width * CH)
        outer_terms = lax.dot_general(picked, right_flat, (((0,), (0,)), ((), ())), preferred_element_type=jnp.float32) * (1.0 / SEQS)
        outer_terms = outer_terms.reshape(block_width, CH, RES, CH).transpose(0, 2, 1, 3).reshape(block_width * RES, CH * CH)
        projected = jnp.dot(outer_terms, weight_full, precision=lax.Precision.HIGHEST) + out_bias
        return projected.reshape(block_width, RES, CZ).astype(jnp.bfloat16)
    blocks = lax.map(row_block, jnp.arange(RES // block_width, dtype=jnp.int32))
    return blocks.reshape(RES, RES, CZ)
```

```python
import functools
import math

import jax
import jax.numpy as jnp
from jax import lax
from jax.experimental import pallas as pl
from jax.experimental.pallas import tpu as pltpu
from jax.sharding import PartitionSpec as P

F32 = jnp.float32
BF16 = jnp.bfloat16
MESH = pl.DeviceIdType.MESH
LANES = 128
SUBLANES = 8


def dot_last(a, b):
    return lax.dot_general(a, b, (((1,), (1,)), ((), ())), preferred_element_type=F32)


def dot(a, b):
    return jnp.dot(a, b, preferred_element_type=F32)


def kernel(
    n_res, n_seq, x_hbm, gain_hbm, wl_hbm, wr_hbm, w_hbm, bias_hbm, out_ref,
    x_ref, gain_ref, wl_ref, wr_ref, w_ref, bias_ref,
    wide_ref, mixed_ref, left_own, left_got, blocks, right_own, right_got, terms,
    early_bytes, late_bytes, load_sem, lrecv_sem, rrecv_sem, ready_sem,
):
    seqs, res, width = x_ref.shape
    ch = wl_ref.shape[0]
    pack = LANES // seqs
    high = ch // pack
    half = n_res // n_seq
    rows = res * high
    inv_count = 1.0 / (seqs * n_seq)
    my_res, my_seq = lax.axis_index("res"), lax.axis_index("seq")
    my_col = my_res // half
    first = my_seq * half
    short = n_res <= 8

    def load(src, dst, n):
        copy = pltpu.make_async_copy(src, dst, load_sem.at[n])
        copy.start()

    def await_bytes(ref, sem):
        pltpu.make_async_copy(ref, ref, sem).wait()

    load(x_hbm, x_ref, 0)
    load(wr_hbm, wr_ref, 0)
    load(gain_hbm, gain_ref, 0)
    load(wl_hbm, wl_ref, 0)

    barrier = pltpu.get_barrier_semaphore()

    def signal(sem, res_at, seq_at):
        pl.semaphore_signal(
            sem, inc=1, device_id={"res": res_at, "seq": seq_at}, device_id_type=MESH
        )

    for k in range(1, n_seq):
        signal(barrier, my_res, lax.rem(my_seq + k, n_seq))

    def greet(res_at, carry):
        for seq_at in range(n_seq):

            @pl.when((res_at > my_res) & ((my_col == seq_at) | (res_at // half == my_seq)))
            def _():
                signal(barrier, res_at, seq_at)

        return carry

    lax.fori_loop(0, n_res, greet, 0, unroll=short)
    near = jnp.minimum(jnp.maximum(my_res - first, 0), half)
    pl.semaphore_wait(barrier, my_res + (n_seq - 1) * near + n_seq - 1)

    def answer(n, carry):
        for seq_at in range(n_seq):

            @pl.when(first + n < my_res)
            def _():
                signal(ready_sem, first + n, seq_at)

        return carry

    lax.fori_loop(0, half, answer, 0, unroll=short)

    await_bytes(early_bytes, load_sem.at[0])
    load(w_hbm, w_ref, 1)
    load(bias_hbm, bias_ref, 1)

    values = x_ref[...].astype(F32).reshape(seqs * res, width)
    packed = values.astype(BF16)
    gained = (wr_ref[...].astype(F32) * gain_ref[...]).astype(BF16)
    product = None
    for n in range(width // LANES):
        at = slice(n * LANES, (n + 1) * LANES)
        part = dot_last(gained[:, at], packed[:, at])
        product = part if product is None else product + part
    weight_sum = jnp.sum(gained.astype(F32), axis=-1, keepdims=True)
    mean = jnp.mean(values, axis=-1, keepdims=True)
    centred = values - mean
    variance = jnp.mean(centred * centred, axis=-1, keepdims=True)
    scale = lax.rsqrt(variance + 1e-05)

    lane = lax.broadcasted_iota(jnp.int32, (high, LANES), 1)
    in_group = [lane % pack == g for g in range(pack)]

    def spread(pieces):
        total = pieces[0]
        for g in range(1, pack):
            total = jnp.where(in_group[g], pieces[g], total)
        return total

    per_row = SUBLANES // res
    blocks_at = lax.broadcasted_iota(jnp.int32, (seqs * res // SUBLANES, SUBLANES, LANES), 0)
    row_at = lax.broadcasted_iota(jnp.int32, (seqs * res // SUBLANES, SUBLANES, LANES), 1)
    lane_at = lax.broadcasted_iota(jnp.int32, (seqs * res // SUBLANES, SUBLANES, LANES), 2)
    own = blocks_at * per_row + row_at // res == lane_at // pack

    def to_lanes(column):
        tall = jnp.where(own, column.reshape(seqs * res // SUBLANES, SUBLANES, 1), 0.0)
        tall = jnp.sum(tall, axis=0)
        total = tall[:res]
        for n in range(1, per_row):
            total = total + tall[n * res : (n + 1) * res]
        return total

    sums = spread(
        [
            jnp.broadcast_to(weight_sum[g * high : (g + 1) * high], (high, LANES))
            for g in range(pack)
        ]
    )
    mean_at, scale_at = to_lanes(mean), to_lanes(scale)
    for j in range(res):
        pieces = []
        for g in range(pack):
            piece = product[g * high : (g + 1) * high]
            shift = (g - j) % LANES
            pieces.append(pltpu.roll(piece, shift, 1) if shift else piece)
        total = (spread(pieces) - mean_at[j : j + 1] * sums) * scale_at[j : j + 1]
        right_own[j * high : (j + 1) * high, :] = total.astype(BF16)

    my_slot = lax.rem(my_res, half)
    away = lax.rem(my_seq - my_col + n_seq, n_seq)
    right_at = right_got.at[away * half + my_slot]

    def send_right(res_at):
        return pltpu.make_async_remote_copy(
            src_ref=right_own,
            dst_ref=right_at,
            send_sem=load_sem.at[0],
            recv_sem=rrecv_sem,
            device_id={"res": res_at, "seq": my_col},
            device_id_type=MESH,
        )

    def lower(res_at, carry):
        @pl.when(res_at < my_res)
        def _():
            send_right(res_at).start()

        return carry

    lax.fori_loop(0, n_res - 1, lower, 0, unroll=short)
    keep = pltpu.make_async_copy(right_own, right_at, rrecv_sem)

    @pl.when(away == 0)
    def _():
        keep.start()

    @pl.when(away != 0)
    def _():
        send_right(my_res).start()

    normed = (centred * scale * gain_ref[...]).astype(BF16)
    wl_wide = jnp.concatenate([wl_ref[...]] * pack, 0)
    left_own[...] = dot_last(normed, wl_wide).astype(BF16)
    await_bytes(late_bytes, load_sem.at[1])
    left_sends = []
    for k in range(1, n_seq):
        copy = pltpu.make_async_remote_copy(
            src_ref=left_own,
            dst_ref=left_got.at[n_seq - k - 1],
            send_sem=load_sem.at[k],
            recv_sem=lrecv_sem.at[n_seq - k - 1],
            device_id={"res": my_res, "seq": lax.rem(my_seq + k, n_seq)},
            device_id_type=MESH,
        )
        copy.start()
        left_sends.append(copy)

    wide_ref[...] = w_ref[...].astype(F32)
    for h in range(high):
        for g in range(pack):
            e = g * high + h
            at = (h * pack + g) * ch
            mixed_ref[at : at + ch, :] = wide_ref[pl.ds(e, ch, stride=ch), :].astype(BF16)

    to_row = lax.broadcasted_iota(jnp.int32, (res * LANES, seqs * res), 0)
    from_row = lax.broadcasted_iota(jnp.int32, (res * LANES, seqs * res), 1)
    picked = (to_row % LANES) // pack * res + to_row // LANES == from_row
    pick = picked.astype(F32).astype(BF16)
    group_at = lax.broadcasted_iota(jnp.int32, (res * LANES, pack * ch), 0) % pack
    copy_at = lax.broadcasted_iota(jnp.int32, (res * LANES, pack * ch), 1) // ch

    def place(part, source):
        spread_out = jnp.where(group_at == copy_at, dot(pick, source), 0.0).astype(BF16)
        for i in range(res):
            blocks[part * LANES : (part + 1) * LANES, i * pack * ch : (i + 1) * pack * ch] = (
                spread_out[i * LANES : (i + 1) * LANES]
            )

    place(0, left_own[...])
    for k in range(1, n_seq):
        left_sends[n_seq - k - 1].wait_recv()
        place(k, left_got[k - 1])

    @pl.when(my_res < n_res - 1)
    def _():
        pl.semaphore_wait(ready_sem, n_res - 1 - my_res)

    def higher(n, carry):
        @pl.when(n + 1 > my_res)
        def _():
            send_right(n + 1).start()

        return carry

    lax.fori_loop(0, n_res - 1, higher, 0, unroll=short)

    await_bytes(right_got, rrecv_sem)
    group = math.gcd(half, 4)

    def columns(n):
        got = jnp.concatenate(
            [
                right_got[pl.ds(part * half + n * group, group)].reshape(group * rows, LANES)
                for part in range(n_seq)
            ],
            1,
        )
        outer = dot(got, blocks[...])
        for i in range(res):
            terms[i] = outer[:, i * LANES : (i + 1) * LANES]
        count = group * res
        lhs = jnp.concatenate(
            [
                jnp.concatenate(
                    [
                        terms[i, pl.ds(h, count, stride=high), :].astype(BF16)
                        for h in range(high)
                    ],
                    1,
                )
                for i in range(res)
            ],
            0,
        )
        result = dot(lhs, mixed_ref[...]) * inv_count + bias_ref[...]
        for i in range(res):
            at = pl.ds(pl.multiple_of(n * count, count), count)
            out_ref[i, at, :] = result[i * count : (i + 1) * count].astype(out_ref.dtype)

    if half == group:
        columns(0)
    else:

        @pl.loop(0, half // group)
        def _(n):
            columns(n)

    for copy in left_sends:
        copy.wait_send()

    @pl.when(away == 0)
    def _():
        await_bytes(right_got.at[pl.ds(0, n_res - 1)], load_sem.at[0])

    @pl.when(away != 0)
    def _():
        await_bytes(right_got, load_sem.at[0])


def on_device(alignment, ln_gain, proj_left, proj_right, out_weight, out_bias):
    n_res, n_seq = lax.axis_size("res"), lax.axis_size("seq")
    seqs, res, width = alignment.shape
    ch = proj_left.shape[1]
    cz = out_weight.shape[1]
    half = n_res // n_seq
    cols = res * half
    pack = LANES // seqs
    rows = res * (ch // pack)
    wide = res * pack * ch
    group = math.gcd(half, 4)
    unit = 2 * LANES * 4
    early = (seqs * res * width + 2 * ch * width) * 2 + width * 4
    late = ch * ch * cz * 2 + cz * 4
    return pl.pallas_call(
        functools.partial(kernel, n_res, n_seq),
        out_shape=pltpu.VMEM((res, cols, cz), BF16),
        in_specs=[pl.BlockSpec(memory_space=pl.ANY)] * 6,
        out_specs=pl.BlockSpec(memory_space=pltpu.VMEM),
        scratch_shapes=[
            pltpu.VMEM((seqs, res, width), BF16),
            pltpu.VMEM((1, width), F32),
            pltpu.VMEM((ch, width), BF16),
            pltpu.VMEM((ch, width), BF16),
            pltpu.VMEM((ch * ch, cz), BF16),
            pltpu.VMEM((1, cz), F32),
            pltpu.VMEM((ch * ch, cz), F32),
            pltpu.VMEM((ch * ch, cz), BF16),
            pltpu.VMEM((res * seqs, pack * ch), BF16),
            pltpu.VMEM((n_seq - 1, res * seqs, pack * ch), BF16),
            pltpu.VMEM((n_seq * LANES, wide), BF16),
            pltpu.VMEM((rows, LANES), BF16),
            pltpu.VMEM((n_res, rows, LANES), BF16),
            pltpu.VMEM((res, group * rows, LANES), F32),
            pltpu.VMEM((early // unit, 2, LANES), F32),
            pltpu.VMEM((late // (unit // 2), 1, LANES), F32),
            pltpu.SemaphoreType.DMA((n_seq,)),
            pltpu.SemaphoreType.DMA((n_seq - 1,)),
            pltpu.SemaphoreType.DMA,
            pltpu.SemaphoreType.REGULAR,
        ],
        compiler_params=pltpu.CompilerParams(collective_id=0, has_side_effects=True),
    )(
        alignment,
        ln_gain.reshape(1, width),
        proj_left.T,
        proj_right.T,
        out_weight,
        out_bias.reshape(1, cz),
    )


def solution(mesh):
    placed = (P(("groups", "seq"), "res", None), P(), P(), P(), P(), P())
    return jax.shard_map(
        on_device,
        mesh=mesh,
        in_specs=placed,
        out_specs=P(("groups", "res"), "seq", None),
        check_vma=False,
    )
```

```python
import functools
import math

import jax
import jax.numpy as jnp
from jax import lax
from jax.experimental import pallas as pl
from jax.experimental.pallas import tpu as pltpu
from jax.sharding import PartitionSpec as P

F32 = jnp.float32
BF16 = jnp.bfloat16
MESH = pl.DeviceIdType.MESH
LANES = 128
SUBLANES = 8


def dot_last(a, b):
    return lax.dot_general(a, b, (((1,), (1,)), ((), ())), preferred_element_type=F32)


def dot(a, b):
    return jnp.dot(a, b, preferred_element_type=F32)


def kernel(
    n_res, n_seq, x_hbm, gain_hbm, wl_hbm, wr_hbm, w_hbm, bias_hbm, out_ref,
    x_ref, gain_ref, wl_ref, wr_ref, w_ref, bias_ref,
    wide_ref, mixed_ref, left_own, left_got, blocks, right_own, right_got, terms,
    early_bytes, late_bytes, load_sem, lrecv_sem, rrecv_sem, ready_sem,
):
    seqs, res, width = x_ref.shape
    ch = wl_ref.shape[0]
    pack = LANES // seqs
    high = ch // pack
    half = n_res // n_seq
    rows = res * high
    inv_count = 1.0 / (seqs * n_seq)
    my_res, my_seq = lax.axis_index("res"), lax.axis_index("seq")
    my_col = my_res // half
    first = my_seq * half
    short = n_res <= 8
    levels = ready_sem.shape[0]
    step = n_res // levels

    def load(src, dst, n):
        copy = pltpu.make_async_copy(src, dst, load_sem.at[n])
        copy.start()

    def await_bytes(ref, sem):
        pltpu.make_async_copy(ref, ref, sem).wait()

    load(x_hbm, x_ref, 0)
    load(wr_hbm, wr_ref, 0)
    load(gain_hbm, gain_ref, 0)
    load(wl_hbm, wl_ref, 0)

    barrier = pltpu.get_barrier_semaphore()

    def signal(sem, res_at, seq_at):
        pl.semaphore_signal(
            sem, inc=1, device_id={"res": res_at, "seq": seq_at}, device_id_type=MESH
        )

    for k in range(1, n_seq):
        signal(barrier, my_res, lax.rem(my_seq + k, n_seq))

    def greet(res_at, carry):
        for seq_at in range(n_seq):

            @pl.when((res_at > my_res) & ((my_col == seq_at) | (res_at // half == my_seq)))
            def _():
                signal(barrier, res_at, seq_at)

        return carry

    lax.fori_loop(0, n_res, greet, 0, unroll=short)
    near = jnp.minimum(jnp.maximum(my_res - first, 0), half)
    pl.semaphore_wait(barrier, my_res + (n_seq - 1) * near + n_seq - 1)

    my_level = my_res // step

    def answer(n, carry):
        for seq_at in range(n_seq):

            @pl.when(first + n < my_res)
            def _():
                signal(ready_sem.at[my_level], first + n, seq_at)

        return carry

    lax.fori_loop(0, half, answer, 0, unroll=short)

    await_bytes(early_bytes, load_sem.at[0])
    load(w_hbm, w_ref, 1)
    load(bias_hbm, bias_ref, 1)

    values = x_ref[...].astype(F32).reshape(seqs * res, width)
    packed = values.astype(BF16)
    gained = (wr_ref[...].astype(F32) * gain_ref[...]).astype(BF16)
    product = None
    for n in range(width // LANES):
        at = slice(n * LANES, (n + 1) * LANES)
        part = dot_last(gained[:, at], packed[:, at])
        product = part if product is None else product + part
    weight_sum = jnp.sum(gained.astype(F32), axis=-1, keepdims=True)
    mean = jnp.mean(values, axis=-1, keepdims=True)
    centred = values - mean
    variance = jnp.mean(centred * centred, axis=-1, keepdims=True)
    scale = lax.rsqrt(variance + 1e-05)

    lane = lax.broadcasted_iota(jnp.int32, (high, LANES), 1)
    in_group = [lane % pack == g for g in range(pack)]

    def spread(pieces):
        total = pieces[0]
        for g in range(1, pack):
            total = jnp.where(in_group[g], pieces[g], total)
        return total

    per_row = SUBLANES // res
    blocks_at = lax.broadcasted_iota(jnp.int32, (seqs * res // SUBLANES, SUBLANES, LANES), 0)
    row_at = lax.broadcasted_iota(jnp.int32, (seqs * res // SUBLANES, SUBLANES, LANES), 1)
    lane_at = lax.broadcasted_iota(jnp.int32, (seqs * res // SUBLANES, SUBLANES, LANES), 2)
    own = blocks_at * per_row + row_at // res == lane_at // pack

    def to_lanes(column):
        tall = jnp.where(own, column.reshape(seqs * res // SUBLANES, SUBLANES, 1), 0.0)
        tall = jnp.sum(tall, axis=0)
        total = tall[:res]
        for n in range(1, per_row):
            total = total + tall[n * res : (n + 1) * res]
        return total

    sums = spread(
        [
            jnp.broadcast_to(weight_sum[g * high : (g + 1) * high], (high, LANES))
            for g in range(pack)
        ]
    )
    mean_at, scale_at = to_lanes(mean), to_lanes(scale)
    for j in range(res):
        pieces = []
        for g in range(pack):
            piece = product[g * high : (g + 1) * high]
            shift = (g - j) % LANES
            pieces.append(pltpu.roll(piece, shift, 1) if shift else piece)
        total = (spread(pieces) - mean_at[j : j + 1] * sums) * scale_at[j : j + 1]
        right_own[j * high : (j + 1) * high, :] = total.astype(BF16)

    my_slot = lax.rem(my_res, half)
    away = lax.rem(my_seq - my_col + n_seq, n_seq)
    right_at = right_got.at[away * half + my_slot]

    def send_right(res_at):
        return pltpu.make_async_remote_copy(
            src_ref=right_own,
            dst_ref=right_at,
            send_sem=load_sem.at[0],
            recv_sem=rrecv_sem,
            device_id={"res": res_at, "seq": my_col},
            device_id_type=MESH,
        )

    def lower(res_at, carry):
        @pl.when(res_at < my_res)
        def _():
            send_right(res_at).start()

        return carry

    lax.fori_loop(0, n_res - 1, lower, 0, unroll=short)
    keep = pltpu.make_async_copy(right_own, right_at, rrecv_sem)

    @pl.when(away == 0)
    def _():
        keep.start()

    @pl.when(away != 0)
    def _():
        send_right(my_res).start()

    normed = (centred * scale * gain_ref[...]).astype(BF16)
    wl_wide = jnp.concatenate([wl_ref[...]] * pack, 0)
    left_own[...] = dot_last(normed, wl_wide).astype(BF16)
    await_bytes(late_bytes, load_sem.at[1])
    left_sends = []
    for k in range(1, n_seq):
        copy = pltpu.make_async_remote_copy(
            src_ref=left_own,
            dst_ref=left_got.at[n_seq - k - 1],
            send_sem=load_sem.at[k],
            recv_sem=lrecv_sem.at[n_seq - k - 1],
            device_id={"res": my_res, "seq": lax.rem(my_seq + k, n_seq)},
            device_id_type=MESH,
        )
        copy.start()
        left_sends.append(copy)

    wide_ref[...] = w_ref[...].astype(F32)
    for h in range(high):
        for g in range(pack):
            e = g * high + h
            at = (h * pack + g) * ch
            mixed_ref[at : at + ch, :] = wide_ref[pl.ds(e, ch, stride=ch), :].astype(BF16)

    to_row = lax.broadcasted_iota(jnp.int32, (res * LANES, seqs * res), 0)
    from_row = lax.broadcasted_iota(jnp.int32, (res * LANES, seqs * res), 1)
    picked = (to_row % LANES) // pack * res + to_row // LANES == from_row
    pick = picked.astype(F32).astype(BF16)
    group_at = lax.broadcasted_iota(jnp.int32, (res * LANES, pack * ch), 0) % pack
    copy_at = lax.broadcasted_iota(jnp.int32, (res * LANES, pack * ch), 1) // ch

    def place(part, source):
        spread_out = jnp.where(group_at == copy_at, dot(pick, source), 0.0).astype(BF16)
        for i in range(res):
            blocks[part * LANES : (part + 1) * LANES, i * pack * ch : (i + 1) * pack * ch] = (
                spread_out[i * LANES : (i + 1) * LANES]
            )

    place(0, left_own[...])
    for k in range(1, n_seq):
        left_sends[n_seq - k - 1].wait_recv()
        place(k, left_got[k - 1])

    for level in range(levels):
        above = jnp.minimum((level + 1) * step - 1 - my_res, step)

        @pl.when(above > 0)
        def _():
            pl.semaphore_wait(ready_sem.at[level], above)

            def higher(n, carry):
                @pl.when(level * step + n > my_res)
                def _():
                    send_right(level * step + n).start()

                return carry

            lax.fori_loop(0, step, higher, 0, unroll=short)

    await_bytes(right_got, rrecv_sem)
    group = math.gcd(half, 4)

    def columns(n):
        got = jnp.concatenate(
            [
                right_got[pl.ds(part * half + n * group, group)].reshape(group * rows, LANES)
                for part in range(n_seq)
            ],
            1,
        )
        outer = dot(got, blocks[...])
        for i in range(res):
            terms[i] = outer[:, i * LANES : (i + 1) * LANES]
        count = group * res
        lhs = jnp.concatenate(
            [
                jnp.concatenate(
                    [
                        terms[i, pl.ds(h, count, stride=high), :].astype(BF16)
                        for h in range(high)
                    ],
                    1,
                )
                for i in range(res)
            ],
            0,
        )
        result = dot(lhs, mixed_ref[...]) * inv_count + bias_ref[...]
        for i in range(res):
            at = pl.ds(pl.multiple_of(n * count, count), count)
            out_ref[i, at, :] = result[i * count : (i + 1) * count].astype(out_ref.dtype)

    if half == group:
        columns(0)
    else:

        @pl.loop(0, half // group)
        def _(n):
            columns(n)

    for copy in left_sends:
        copy.wait_send()

    @pl.when(away == 0)
    def _():
        await_bytes(right_got.at[pl.ds(0, n_res - 1)], load_sem.at[0])

    @pl.when(away != 0)
    def _():
        await_bytes(right_got, load_sem.at[0])


def on_device(alignment, ln_gain, proj_left, proj_right, out_weight, out_bias):
    n_res, n_seq = lax.axis_size("res"), lax.axis_size("seq")
    seqs, res, width = alignment.shape
    ch = proj_left.shape[1]
    cz = out_weight.shape[1]
    half = n_res // n_seq
    cols = res * half
    pack = LANES // seqs
    rows = res * (ch // pack)
    wide = res * pack * ch
    group = math.gcd(half, 4)
    unit = 2 * LANES * 4
    early = (seqs * res * width + 2 * ch * width) * 2 + width * 4
    late = ch * ch * cz * 2 + cz * 4
    return pl.pallas_call(
        functools.partial(kernel, n_res, n_seq),
        out_shape=pltpu.VMEM((res, cols, cz), BF16),
        in_specs=[pl.BlockSpec(memory_space=pl.ANY)] * 6,
        out_specs=pl.BlockSpec(memory_space=pltpu.VMEM),
        scratch_shapes=[
            pltpu.VMEM((seqs, res, width), BF16),
            pltpu.VMEM((1, width), F32),
            pltpu.VMEM((ch, width), BF16),
            pltpu.VMEM((ch, width), BF16),
            pltpu.VMEM((ch * ch, cz), BF16),
            pltpu.VMEM((1, cz), F32),
            pltpu.VMEM((ch * ch, cz), F32),
            pltpu.VMEM((ch * ch, cz), BF16),
            pltpu.VMEM((res * seqs, pack * ch), BF16),
            pltpu.VMEM((n_seq - 1, res * seqs, pack * ch), BF16),
            pltpu.VMEM((n_seq * LANES, wide), BF16),
            pltpu.VMEM((rows, LANES), BF16),
            pltpu.VMEM((n_res, rows, LANES), BF16),
            pltpu.VMEM((res, group * rows, LANES), F32),
            pltpu.VMEM((early // unit, 2, LANES), F32),
            pltpu.VMEM((late // (unit // 2), 1, LANES), F32),
            pltpu.SemaphoreType.DMA((n_seq,)),
            pltpu.SemaphoreType.DMA((n_seq - 1,)),
            pltpu.SemaphoreType.DMA,
            pltpu.SemaphoreType.REGULAR((2 * n_seq,)),
        ],
        compiler_params=pltpu.CompilerParams(collective_id=0, has_side_effects=True),
    )(
        alignment,
        ln_gain.reshape(1, width),
        proj_left.T,
        proj_right.T,
        out_weight,
        out_bias.reshape(1, cz),
    )


def solution(mesh):
    placed = (P(("groups", "seq"), "res", None), P(), P(), P(), P(), P())
    return jax.shard_map(
        on_device,
        mesh=mesh,
        in_specs=placed,
        out_specs=P(("groups", "res"), "seq", None),
        check_vma=False,
    )
```

```python
import functools
import math

import jax
import jax.numpy as jnp
from jax import lax
from jax.experimental import pallas as pl
from jax.experimental.pallas import tpu as pltpu
from jax.sharding import PartitionSpec as P

F32 = jnp.float32
BF16 = jnp.bfloat16
MESH = pl.DeviceIdType.MESH
LANES = 128
SUBLANES = 8


def dot_last(a, b):
    return lax.dot_general(a, b, (((1,), (1,)), ((), ())), preferred_element_type=F32)


def dot(a, b):
    return jnp.dot(a, b, preferred_element_type=F32)


def kernel(
    n_res, n_seq, x_hbm, gain_hbm, wl_hbm, wr_hbm, w_hbm, bias_hbm, out_ref,
    x_ref, gain_ref, wl_ref, wr_ref, w_ref, bias_ref,
    wide_ref, mixed_ref, left_own, left_got, blocks, right_own, right_got, tall,
    early_bytes, late_bytes, lrecv_sem, rrecv_sem, ready_sem, load_sem,
):
    seqs, res, width = x_ref.shape
    ch = wl_ref.shape[0]
    cz = bias_ref.shape[1]
    pack = LANES // seqs
    high = ch // pack
    half = n_res // n_seq
    rows = res * high
    inv_count = 1.0 / (seqs * n_seq)
    my_res, my_seq = lax.axis_index("res"), lax.axis_index("seq")
    my_col = my_res // half
    first = my_seq * half
    short = n_res <= 8
    levels = ready_sem.shape[0]
    step = n_res // levels

    def load(src, dst, n):
        copy = pltpu.make_async_copy(src, dst, load_sem.at[n])
        copy.start()

    def await_bytes(ref, sem):
        pltpu.make_async_copy(ref, ref, sem).wait()

    for n in range(4):
        at = pl.ds(n * (seqs // 4), seqs // 4)
        load(x_hbm.at[at], x_ref.at[at], 0)
    load(wr_hbm, wr_ref, 0)
    load(gain_hbm, gain_ref, 0)
    load(wl_hbm, wl_ref, 0)

    barrier = pltpu.get_barrier_semaphore()

    def signal(sem, res_at, seq_at):
        pl.semaphore_signal(
            sem, inc=1, device_id={"res": res_at, "seq": seq_at}, device_id_type=MESH
        )

    for k in range(1, n_seq):
        signal(barrier, my_res, lax.rem(my_seq + k, n_seq))

    def greet(res_at, carry):
        for seq_at in range(n_seq):

            @pl.when((res_at > my_res) & ((my_col == seq_at) | (res_at // half == my_seq)))
            def _():
                signal(barrier, res_at, seq_at)

        return carry

    lax.fori_loop(0, n_res, greet, 0, unroll=short)
    near = jnp.minimum(jnp.maximum(my_res - first, 0), half)
    pl.semaphore_wait(barrier, my_res + (n_seq - 1) * near + n_seq - 1)

    my_level = my_res // step

    def answer(n, carry):
        for seq_at in range(n_seq):

            @pl.when(first + n < my_res)
            def _():
                signal(ready_sem.at[my_level], first + n, seq_at)

        return carry

    lax.fori_loop(0, half, answer, 0, unroll=short)

    await_bytes(early_bytes, load_sem.at[0])
    load(w_hbm, w_ref, 1)
    load(bias_hbm, bias_ref, 1)

    values = x_ref[...].astype(F32).reshape(seqs * res, width)
    packed = values.astype(BF16)
    gained = (wr_ref[...].astype(F32) * gain_ref[...]).astype(BF16)
    product = None
    for n in range(width // LANES):
        at = slice(n * LANES, (n + 1) * LANES)
        if n % 2 == 0:
            part = dot_last(gained[:, at], packed[:, at])
            product = part if product is None else product + part
        else:
            product = product - dot_last(-gained[:, at], packed[:, at])
    weight_sum = jnp.sum(gained.astype(F32), axis=-1, keepdims=True)
    mean = jnp.mean(values, axis=-1, keepdims=True)
    centred = values - mean
    variance = jnp.mean(centred * centred, axis=-1, keepdims=True)
    scale = lax.rsqrt(variance + 1e-05)

    lane = lax.broadcasted_iota(jnp.int32, (high, LANES), 1)
    in_group = [lane % pack == g for g in range(pack)]

    def spread(pieces):
        total = pieces[0]
        for g in range(1, pack):
            total = jnp.where(in_group[g], pieces[g], total)
        return total

    per_row = SUBLANES // res
    blocks_at = lax.broadcasted_iota(jnp.int32, (seqs * res // SUBLANES, SUBLANES, LANES), 0)
    row_at = lax.broadcasted_iota(jnp.int32, (seqs * res // SUBLANES, SUBLANES, LANES), 1)
    lane_at = lax.broadcasted_iota(jnp.int32, (seqs * res // SUBLANES, SUBLANES, LANES), 2)
    own = blocks_at * per_row + row_at // res == lane_at // pack

    def to_lanes(column):
        tall = jnp.where(own, column.reshape(seqs * res // SUBLANES, SUBLANES, 1), 0.0)
        tall = jnp.sum(tall, axis=0)
        total = tall[:res]
        for n in range(1, per_row):
            total = total + tall[n * res : (n + 1) * res]
        return total

    sums = spread(
        [
            jnp.broadcast_to(weight_sum[g * high : (g + 1) * high], (high, LANES))
            for g in range(pack)
        ]
    )
    mean_at, scale_at = to_lanes(mean), to_lanes(scale)
    for j in range(res):
        pieces = []
        for g in range(pack):
            piece = product[g * high : (g + 1) * high]
            shift = (g - j) % LANES
            pieces.append(pltpu.roll(piece, shift, 1) if shift else piece)
        total = (spread(pieces) - mean_at[j : j + 1] * sums) * scale_at[j : j + 1]
        tall[pl.ds(j, high, stride=res), :] = total
    right_own[...] = tall[...].astype(BF16)

    my_slot = lax.rem(my_res, half)
    away = lax.rem(my_seq - my_col + n_seq, n_seq)
    right_at = right_got.at[away * half + my_slot]

    def send_right(res_at):
        return pltpu.make_async_remote_copy(
            src_ref=right_own,
            dst_ref=right_at,
            send_sem=load_sem.at[0],
            recv_sem=rrecv_sem,
            device_id={"res": res_at, "seq": my_col},
            device_id_type=MESH,
        )

    def lower(res_at, carry):
        @pl.when(res_at < my_res)
        def _():
            send_right(res_at).start()

        return carry

    lax.fori_loop(0, n_res - 1, lower, 0, unroll=short)
    keep = pltpu.make_async_copy(right_own, right_at, rrecv_sem)

    @pl.when(away == 0)
    def _():
        keep.start()

    @pl.when(away != 0)
    def _():
        send_right(my_res).start()

    normed = (centred * scale * gain_ref[...]).astype(BF16)
    wl_wide = jnp.concatenate([wl_ref[...]] * pack, 0)
    left_own[...] = dot_last(normed, wl_wide).astype(BF16)
    await_bytes(late_bytes, load_sem.at[1])
    left_sends = []
    for k in range(1, n_seq):
        copy = pltpu.make_async_remote_copy(
            src_ref=left_own,
            dst_ref=left_got.at[n_seq - k - 1],
            send_sem=load_sem.at[k],
            recv_sem=lrecv_sem.at[n_seq - k - 1],
            device_id={"res": my_res, "seq": lax.rem(my_seq + k, n_seq)},
            device_id_type=MESH,
        )
        copy.start()
        left_sends.append(copy)

    wide_ref[...] = w_ref[...].astype(F32)
    for h in range(high):
        for g in range(pack):
            e = g * high + h
            at = (h // per_row * pack + g) * ch
            out_at = h % per_row * cz
            mixed_ref[at : at + ch, out_at : out_at + cz] = wide_ref[
                pl.ds(e, ch, stride=ch), :
            ].astype(BF16)

    to_row = lax.broadcasted_iota(jnp.int32, (res * LANES, seqs * res), 0)
    from_row = lax.broadcasted_iota(jnp.int32, (res * LANES, seqs * res), 1)
    picked = (to_row % LANES) // pack * res + to_row // LANES == from_row
    pick = picked.astype(F32).astype(BF16)
    group_at = lax.broadcasted_iota(jnp.int32, (LANES, pack * ch), 0) % pack
    copy_at = lax.broadcasted_iota(jnp.int32, (LANES, pack * ch), 1) // ch

    def place(part, source):
        for i in range(res):
            own_rows = pick[i * LANES : (i + 1) * LANES]
            blocks[part * LANES : (part + 1) * LANES, i * pack * ch : (i + 1) * pack * ch] = (
                jnp.where(group_at == copy_at, dot(own_rows, source), 0.0).astype(BF16)
            )

    place(0, left_own[...])
    for k in range(1, n_seq):
        left_sends[n_seq - k - 1].wait_recv()
        place(k, left_got[k - 1])

    for level in range(levels):
        above = jnp.minimum((level + 1) * step - 1 - my_res, step)

        @pl.when(above > 0)
        def _():
            pl.semaphore_wait(ready_sem.at[level], above)

            def higher(n, carry):
                @pl.when(level * step + n > my_res)
                def _():
                    send_right(level * step + n).start()

                return carry

            lax.fori_loop(0, step, higher, 0, unroll=short)

    await_bytes(right_got, rrecv_sem)
    group = math.gcd(half, 4)

    tiles = high // per_row

    def columns(n):
        got = jnp.concatenate(
            [
                jnp.concatenate(
                    [
                        right_got[
                            pl.ds(part * half + n * group, group),
                            tile * SUBLANES : (tile + 1) * SUBLANES,
                        ].reshape(group * SUBLANES, LANES)
                        for part in range(n_seq)
                    ],
                    1,
                )
                for tile in range(tiles)
            ],
            0,
        )
        outer = dot(got, blocks[...])
        count = group * SUBLANES
        lhs = jnp.concatenate(
            [
                jnp.concatenate(
                    [
                        outer[tile * count : (tile + 1) * count, i * LANES : (i + 1) * LANES]
                        for tile in range(tiles)
                    ],
                    1,
                )
                for i in range(res)
            ],
            0,
        ).astype(BF16)
        pairs = dot(lhs, mixed_ref[...])
        for i in range(res):
            for slot in range(0, group, per_row):
                pieces = []
                for q in range(per_row):
                    at = i * count + (slot + q) * SUBLANES
                    piece = pairs[at : at + res, :cz]
                    for h in range(1, per_row):
                        piece = piece + pairs[at + h * res : at + (h + 1) * res, h * cz : (h + 1) * cz]
                    pieces.append(piece)
                result = jnp.concatenate(pieces, 0) * inv_count + bias_ref[...]
                at = pl.ds(pl.multiple_of((n * group + slot) * res, SUBLANES), SUBLANES)
                out_ref[i, at, :] = result.astype(out_ref.dtype)

    if half == group:
        columns(0)
    else:

        @pl.loop(0, half // group)
        def _(n):
            columns(n)

    for copy in left_sends:
        copy.wait_send()

    @pl.when(away == 0)
    def _():
        await_bytes(right_got.at[pl.ds(0, n_res - 1)], load_sem.at[0])

    @pl.when(away != 0)
    def _():
        await_bytes(right_got, load_sem.at[0])


def scoped(n_res, n_seq, *refs):
    pl.run_scoped(
        functools.partial(kernel, n_res, n_seq, *refs), pltpu.SemaphoreType.DMA((n_seq,))
    )


def on_device(alignment, ln_gain, proj_left, proj_right, out_weight, out_bias):
    n_res, n_seq = lax.axis_size("res"), lax.axis_size("seq")
    seqs, res, width = alignment.shape
    ch = proj_left.shape[1]
    cz = out_weight.shape[1]
    half = n_res // n_seq
    cols = res * half
    pack = LANES // seqs
    rows = res * (ch // pack)
    wide = res * pack * ch
    group = math.gcd(half, 4)
    per_row = SUBLANES // res
    unit = 2 * LANES * 4
    early = (seqs * res * width + 2 * ch * width) * 2 + width * 4
    late = ch * ch * cz * 2 + cz * 4
    return pl.pallas_call(
        functools.partial(scoped, n_res, n_seq),
        out_shape=pltpu.VMEM((res, cols, cz), BF16),
        in_specs=[pl.BlockSpec(memory_space=pl.ANY)] * 6,
        out_specs=pl.BlockSpec(memory_space=pltpu.VMEM),
        scratch_shapes=[
            pltpu.VMEM((seqs, res, width), BF16),
            pltpu.VMEM((1, width), F32),
            pltpu.VMEM((ch, width), BF16),
            pltpu.VMEM((ch, width), BF16),
            pltpu.VMEM((ch * ch, cz), BF16),
            pltpu.VMEM((1, cz), F32),
            pltpu.VMEM((ch * ch, cz), F32),
            pltpu.VMEM((ch * ch // per_row, per_row * cz), BF16),
            pltpu.VMEM((res * seqs, pack * ch), BF16),
            pltpu.VMEM((n_seq - 1, res * seqs, pack * ch), BF16),
            pltpu.VMEM((n_seq * LANES, wide), BF16),
            pltpu.VMEM((rows, LANES), BF16),
            pltpu.VMEM((n_res, rows, LANES), BF16),
            pltpu.VMEM((rows, LANES), F32),
            pltpu.VMEM((early // unit, 2, LANES), F32),
            pltpu.VMEM((late // (unit // 2), 1, LANES), F32),
            pltpu.SemaphoreType.DMA((n_seq - 1,)),
            pltpu.SemaphoreType.DMA,
            pltpu.SemaphoreType.REGULAR((2 * n_seq,)),
        ],
        compiler_params=pltpu.CompilerParams(collective_id=0, has_side_effects=True),
    )(
        alignment,
        ln_gain.reshape(1, width),
        proj_left.T,
        proj_right.T,
        out_weight,
        out_bias.reshape(1, cz),
    )


def solution(mesh):
    placed = (P(("groups", "seq"), "res", None), P(), P(), P(), P(), P())
    return jax.shard_map(
        on_device,
        mesh=mesh,
        in_specs=placed,
        out_specs=P(("groups", "res"), "seq", None),
        check_vma=False,
    )
```

```python
import functools
import math

import jax
import jax.numpy as jnp
from jax import lax
from jax.experimental import pallas as pl
from jax.experimental.pallas import tpu as pltpu
from jax.sharding import PartitionSpec as P

F32 = jnp.float32
BF16 = jnp.bfloat16
MESH = pl.DeviceIdType.MESH
LANES = 128
SUBLANES = 8


def dot_last(a, b):
    return lax.dot_general(a, b, (((1,), (1,)), ((), ())), preferred_element_type=F32)


def dot(a, b):
    return jnp.dot(a, b, preferred_element_type=F32)


def kernel(
    n_res, n_seq, x_hbm, gain_hbm, wl_hbm, wr_hbm, w_hbm, bias_hbm, out_ref,
    x_ref, gain_ref, wl_ref, wr_ref, w_ref, bias_ref,
    wide_ref, mixed_ref, left_own, left_got, blocks, right_own, right_got, tall,
    early_bytes, late_bytes, load_sem, lrecv_sem, rrecv_sem, ready_sem,
):
    seqs, res, width = x_ref.shape
    ch = wl_ref.shape[0]
    cz = bias_ref.shape[1]
    pack = LANES // seqs
    high = ch // pack
    half = n_res // n_seq
    rows = res * high
    inv_count = 1.0 / (seqs * n_seq)
    my_res, my_seq = lax.axis_index("res"), lax.axis_index("seq")
    my_col = my_res // half
    first = my_seq * half
    short = n_res <= 8
    levels = ready_sem.shape[0]
    step = n_res // levels

    def load(src, dst, n):
        copy = pltpu.make_async_copy(src, dst, load_sem.at[n])
        copy.start()

    def await_bytes(ref, sem):
        pltpu.make_async_copy(ref, ref, sem).wait()

    for n in range(4):
        at = pl.ds(n * (seqs // 4), seqs // 4)
        load(x_hbm.at[at], x_ref.at[at], 0)
    load(wr_hbm, wr_ref, 0)
    load(gain_hbm, gain_ref, 0)
    load(wl_hbm, wl_ref, n_seq)

    barrier = pltpu.get_barrier_semaphore()

    def signal(sem, res_at, seq_at):
        pl.semaphore_signal(
            sem, inc=1, device_id={"res": res_at, "seq": seq_at}, device_id_type=MESH
        )

    for k in range(1, n_seq):
        signal(barrier, my_res, lax.rem(my_seq + k, n_seq))

    def greet(res_at, carry):
        for seq_at in range(n_seq):

            @pl.when((res_at > my_res) & ((my_col == seq_at) | (res_at // half == my_seq)))
            def _():
                signal(barrier, res_at, seq_at)

        return carry

    lax.fori_loop(0, n_res, greet, 0, unroll=short)
    near = jnp.minimum(jnp.maximum(my_res - first, 0), half)
    pl.semaphore_wait(barrier, my_res + (n_seq - 1) * near + n_seq - 1)

    my_level = my_res // step

    def answer(n, carry):
        for seq_at in range(n_seq):

            @pl.when(first + n < my_res)
            def _():
                signal(ready_sem.at[my_level], first + n, seq_at)

        return carry

    lax.fori_loop(0, half, answer, 0, unroll=short)

    await_bytes(early_bytes, load_sem.at[0])
    load(w_hbm, w_ref, 1)
    load(bias_hbm, bias_ref, 1)

    values = x_ref[...].astype(F32).reshape(seqs * res, width)
    packed = values.astype(BF16)
    gained = (wr_ref[...].astype(F32) * gain_ref[...]).astype(BF16)
    product = None
    for n in range(width // LANES):
        at = slice(n * LANES, (n + 1) * LANES)
        if n % 2 == 0:
            part = dot_last(gained[:, at], packed[:, at])
            product = part if product is None else product + part
        else:
            product = product - dot_last(-gained[:, at], packed[:, at])
    weight_sum = jnp.sum(gained.astype(F32), axis=-1, keepdims=True)
    mean = jnp.mean(values, axis=-1, keepdims=True)
    centred = values - mean
    variance = jnp.mean(centred * centred, axis=-1, keepdims=True)
    scale = lax.rsqrt(variance + 1e-05)

    lane = lax.broadcasted_iota(jnp.int32, (high, LANES), 1)
    in_group = [lane % pack == g for g in range(pack)]

    def spread(pieces):
        total = pieces[0]
        for g in range(1, pack):
            total = jnp.where(in_group[g], pieces[g], total)
        return total

    per_row = SUBLANES // res
    blocks_at = lax.broadcasted_iota(jnp.int32, (seqs * res // SUBLANES, SUBLANES, LANES), 0)
    row_at = lax.broadcasted_iota(jnp.int32, (seqs * res // SUBLANES, SUBLANES, LANES), 1)
    lane_at = lax.broadcasted_iota(jnp.int32, (seqs * res // SUBLANES, SUBLANES, LANES), 2)
    own = blocks_at * per_row + row_at // res == lane_at // pack

    def to_lanes(column):
        tall = jnp.where(own, column.reshape(seqs * res // SUBLANES, SUBLANES, 1), 0.0)
        tall = jnp.sum(tall, axis=0)
        total = tall[:res]
        for n in range(1, per_row):
            total = total + tall[n * res : (n + 1) * res]
        return total

    sums = spread(
        [
            jnp.broadcast_to(weight_sum[g * high : (g + 1) * high], (high, LANES))
            for g in range(pack)
        ]
    )
    mean_at, scale_at = to_lanes(mean), to_lanes(scale)
    for j in range(res):
        pieces = []
        for g in range(pack):
            piece = product[g * high : (g + 1) * high]
            shift = (g - j) % LANES
            pieces.append(pltpu.roll(piece, shift, 1) if shift else piece)
        total = (spread(pieces) - mean_at[j : j + 1] * sums) * scale_at[j : j + 1]
        tall[pl.ds(j, high, stride=res), :] = total
    right_own[...] = tall[...].astype(BF16)

    my_slot = lax.rem(my_res, half)
    away = lax.rem(my_seq - my_col + n_seq, n_seq)
    right_at = right_got.at[away * half + my_slot]

    def send_right(res_at):
        return pltpu.make_async_remote_copy(
            src_ref=right_own,
            dst_ref=right_at,
            send_sem=load_sem.at[0],
            recv_sem=rrecv_sem,
            device_id={"res": res_at, "seq": my_col},
            device_id_type=MESH,
        )

    def lower(res_at, carry):
        @pl.when(res_at < my_res)
        def _():
            send_right(res_at).start()

        return carry

    lax.fori_loop(0, n_res - 1, lower, 0, unroll=short)
    keep = pltpu.make_async_copy(right_own, right_at, rrecv_sem)

    @pl.when(away == 0)
    def _():
        keep.start()

    @pl.when(away != 0)
    def _():
        send_right(my_res).start()

    await_bytes(wl_ref, load_sem.at[n_seq])
    normed = (centred * scale * gain_ref[...]).astype(BF16)
    wl_wide = jnp.concatenate([wl_ref[...]] * pack, 0)
    left_own[...] = dot_last(normed, wl_wide).astype(BF16)
    await_bytes(late_bytes, load_sem.at[1])
    left_sends = []
    for k in range(1, n_seq):
        copy = pltpu.make_async_remote_copy(
            src_ref=left_own,
            dst_ref=left_got.at[n_seq - k - 1],
            send_sem=load_sem.at[k],
            recv_sem=lrecv_sem.at[n_seq - k - 1],
            device_id={"res": my_res, "seq": lax.rem(my_seq + k, n_seq)},
            device_id_type=MESH,
        )
        copy.start()
        left_sends.append(copy)

    wide_ref[...] = w_ref[...].astype(F32)
    for h in range(high):
        for g in range(pack):
            e = g * high + h
            at = (h // per_row * pack + g) * ch
            out_at = h % per_row * cz
            mixed_ref[at : at + ch, out_at : out_at + cz] = wide_ref[
                pl.ds(e, ch, stride=ch), :
            ].astype(BF16)

    to_row = lax.broadcasted_iota(jnp.int32, (res * LANES, seqs * res), 0)
    from_row = lax.broadcasted_iota(jnp.int32, (res * LANES, seqs * res), 1)
    picked = (to_row % LANES) // pack * res + to_row // LANES == from_row
    pick = picked.astype(F32).astype(BF16)
    group_at = lax.broadcasted_iota(jnp.int32, (LANES, pack * ch), 0) % pack
    copy_at = lax.broadcasted_iota(jnp.int32, (LANES, pack * ch), 1) // ch

    def place(part, source):
        for i in range(res):
            own_rows = pick[i * LANES : (i + 1) * LANES]
            blocks[part * LANES : (part + 1) * LANES, i * pack * ch : (i + 1) * pack * ch] = (
                jnp.where(group_at == copy_at, dot(own_rows, source), 0.0).astype(BF16)
            )

    place(0, left_own[...])
    for k in range(1, n_seq):
        left_sends[n_seq - k - 1].wait_recv()
        place(k, left_got[k - 1])

    for level in range(levels):
        above = jnp.minimum((level + 1) * step - 1 - my_res, step)

        @pl.when(above > 0)
        def _():
            pl.semaphore_wait(ready_sem.at[level], above)

            def higher(n, carry):
                @pl.when(level * step + n > my_res)
                def _():
                    send_right(level * step + n).start()

                return carry

            lax.fori_loop(0, step, higher, 0, unroll=short)

    await_bytes(right_got, rrecv_sem)
    group = math.gcd(half, 4)

    tiles = high // per_row

    def columns(n):
        got = jnp.concatenate(
            [
                jnp.concatenate(
                    [
                        right_got[
                            pl.ds(part * half + n * group, group),
                            tile * SUBLANES : (tile + 1) * SUBLANES,
                        ].reshape(group * SUBLANES, LANES)
                        for part in range(n_seq)
                    ],
                    1,
                )
                for tile in range(tiles)
            ],
            0,
        )
        outer = dot(got, blocks[...])
        count = group * SUBLANES
        lhs = jnp.concatenate(
            [
                jnp.concatenate(
                    [
                        outer[tile * count : (tile + 1) * count, i * LANES : (i + 1) * LANES]
                        for tile in range(tiles)
                    ],
                    1,
                )
                for i in range(res)
            ],
            0,
        ).astype(BF16)
        pairs = dot(lhs, mixed_ref[...])
        for i in range(res):
            for slot in range(0, group, per_row):
                pieces = []
                for q in range(per_row):
                    at = i * count + (slot + q) * SUBLANES
                    piece = pairs[at : at + res, :cz]
                    for h in range(1, per_row):
                        piece = piece + pairs[at + h * res : at + (h + 1) * res, h * cz : (h + 1) * cz]
                    pieces.append(piece)
                result = jnp.concatenate(pieces, 0) * inv_count + bias_ref[...]
                at = pl.ds(pl.multiple_of((n * group + slot) * res, SUBLANES), SUBLANES)
                out_ref[i, at, :] = result.astype(out_ref.dtype)

    if half == group:
        columns(0)
    else:

        @pl.loop(0, half // group)
        def _(n):
            columns(n)

    for copy in left_sends:
        copy.wait_send()

    @pl.when(away == 0)
    def _():
        await_bytes(right_got.at[pl.ds(0, n_res - 1)], load_sem.at[0])

    @pl.when(away != 0)
    def _():
        await_bytes(right_got, load_sem.at[0])


def scoped(n_res, n_seq, *refs):
    pl.run_scoped(
        functools.partial(kernel, n_res, n_seq, *refs),
        pltpu.SemaphoreType.DMA((n_seq + 1,)),
        pltpu.SemaphoreType.DMA((n_seq - 1,)),
        pltpu.SemaphoreType.DMA,
        pltpu.SemaphoreType.REGULAR((2 * n_seq,)),
    )


def on_device(alignment, ln_gain, proj_left, proj_right, out_weight, out_bias):
    n_res, n_seq = lax.axis_size("res"), lax.axis_size("seq")
    seqs, res, width = alignment.shape
    ch = proj_left.shape[1]
    cz = out_weight.shape[1]
    half = n_res // n_seq
    cols = res * half
    pack = LANES // seqs
    rows = res * (ch // pack)
    wide = res * pack * ch
    group = math.gcd(half, 4)
    per_row = SUBLANES // res
    unit = 2 * LANES * 4
    early = (seqs * res * width + ch * width) * 2 + width * 4
    late = ch * ch * cz * 2 + cz * 4
    return pl.pallas_call(
        functools.partial(scoped, n_res, n_seq),
        out_shape=pltpu.VMEM((res, cols, cz), BF16),
        in_specs=[pl.BlockSpec(memory_space=pl.ANY)] * 6,
        out_specs=pl.BlockSpec(memory_space=pltpu.VMEM),
        scratch_shapes=[
            pltpu.VMEM((seqs, res, width), BF16),
            pltpu.VMEM((1, width), F32),
            pltpu.VMEM((ch, width), BF16),
            pltpu.VMEM((ch, width), BF16),
            pltpu.VMEM((ch * ch, cz), BF16),
            pltpu.VMEM((1, cz), F32),
            pltpu.VMEM((ch * ch, cz), F32),
            pltpu.VMEM((ch * ch // per_row, per_row * cz), BF16),
            pltpu.VMEM((res * seqs, pack * ch), BF16),
            pltpu.VMEM((n_seq - 1, res * seqs, pack * ch), BF16),
            pltpu.VMEM((n_seq * LANES, wide), BF16),
            pltpu.VMEM((rows, LANES), BF16),
            pltpu.VMEM((n_res, rows, LANES), BF16),
            pltpu.VMEM((rows, LANES), F32),
            pltpu.VMEM((early // unit, 2, LANES), F32),
            pltpu.VMEM((late // (unit // 2), 1, LANES), F32),
        ],
        compiler_params=pltpu.CompilerParams(collective_id=0, has_side_effects=True),
    )(
        alignment,
        ln_gain.reshape(1, width),
        proj_left.T,
        proj_right.T,
        out_weight,
        out_bias.reshape(1, cz),
    )


def solution(mesh):
    placed = (P(("groups", "seq"), "res", None), P(), P(), P(), P(), P())
    return jax.shard_map(
        on_device,
        mesh=mesh,
        in_specs=placed,
        out_specs=P(("groups", "res"), "seq", None),
        check_vma=False,
    )
```

```python
import functools
import math

import jax
import jax.numpy as jnp
from jax import lax
from jax.experimental import pallas as pl
from jax.experimental.pallas import tpu as pltpu
from jax.sharding import PartitionSpec as P

F32 = jnp.float32
BF16 = jnp.bfloat16
MESH = pl.DeviceIdType.MESH
LANES = 128
SUBLANES = 8


def dot_last(a, b):
    return lax.dot_general(a, b, (((1,), (1,)), ((), ())), preferred_element_type=F32)


def dot(a, b):
    return jnp.dot(a, b, preferred_element_type=F32)


def kernel(
    n_res, n_seq, x_hbm, gain_hbm, wl_hbm, wr_hbm, w_hbm, bias_hbm, out_ref,
    x_ref, gain_ref, wl_ref, wr_ref, w_ref, bias_ref,
    wide_ref, mixed_ref, left_own, left_got, blocks, right_own, right_got, tall,
    early_bytes, late_bytes, load_sem, lrecv_sem, rrecv_sem, ready_sem,
):
    seqs, res, width = x_ref.shape
    ch = wl_ref.shape[0]
    cz = bias_ref.shape[1]
    pack = LANES // seqs
    high = ch // pack
    half = n_res // n_seq
    rows = res * high
    inv_count = 1.0 / (seqs * n_seq)
    my_res, my_seq = lax.axis_index("res"), lax.axis_index("seq")
    my_col = my_res // half
    first = my_seq * half
    short = n_res <= 8
    levels = ready_sem.shape[0]
    step = n_res // levels

    def load(src, dst, n):
        copy = pltpu.make_async_copy(src, dst, load_sem.at[n])
        copy.start()

    def await_bytes(ref, sem):
        pltpu.make_async_copy(ref, ref, sem).wait()

    for n in range(4):
        at = pl.ds(n * (seqs // 4), seqs // 4)
        load(x_hbm.at[at], x_ref.at[at], 0)
    load(wr_hbm, wr_ref, 0)
    load(gain_hbm, gain_ref, 0)
    load(wl_hbm, wl_ref, n_seq)
    load(w_hbm, w_ref, 1)
    load(bias_hbm, bias_ref, 1)

    barrier = pltpu.get_barrier_semaphore()

    def signal(sem, res_at, seq_at):
        pl.semaphore_signal(
            sem, inc=1, device_id={"res": res_at, "seq": seq_at}, device_id_type=MESH
        )

    for k in range(1, n_seq):
        signal(barrier, my_res, lax.rem(my_seq + k, n_seq))

    def greet(res_at, carry):
        for seq_at in range(n_seq):

            @pl.when((res_at > my_res) & ((my_col == seq_at) | (res_at // half == my_seq)))
            def _():
                signal(barrier, res_at, seq_at)

        return carry

    lax.fori_loop(0, n_res, greet, 0, unroll=short)
    near = jnp.minimum(jnp.maximum(my_res - first, 0), half)
    pl.semaphore_wait(barrier, my_res + (n_seq - 1) * near + n_seq - 1)

    my_level = my_res // step

    def answer(n, carry):
        for seq_at in range(n_seq):

            @pl.when(first + n < my_res)
            def _():
                signal(ready_sem.at[my_level], first + n, seq_at)

        return carry

    lax.fori_loop(0, half, answer, 0, unroll=short)

    await_bytes(early_bytes, load_sem.at[0])

    values = x_ref[...].astype(F32).reshape(seqs * res, width)
    packed = values.astype(BF16)
    gained = (wr_ref[...].astype(F32) * gain_ref[...]).astype(BF16)
    product = None
    for n in range(width // LANES):
        at = slice(n * LANES, (n + 1) * LANES)
        if n % 2 == 0:
            part = dot_last(gained[:, at], packed[:, at])
            product = part if product is None else product + part
        else:
            product = product - dot_last(-gained[:, at], packed[:, at])
    weight_sum = jnp.sum(gained.astype(F32), axis=-1, keepdims=True)
    mean = jnp.mean(values, axis=-1, keepdims=True)
    centred = values - mean
    variance = jnp.mean(centred * centred, axis=-1, keepdims=True)
    scale = lax.rsqrt(variance + 1e-05)

    lane = lax.broadcasted_iota(jnp.int32, (high, LANES), 1)
    in_group = [lane % pack == g for g in range(pack)]

    def spread(pieces):
        total = pieces[0]
        for g in range(1, pack):
            total = jnp.where(in_group[g], pieces[g], total)
        return total

    per_row = SUBLANES // res
    blocks_at = lax.broadcasted_iota(jnp.int32, (seqs * res // SUBLANES, SUBLANES, LANES), 0)
    row_at = lax.broadcasted_iota(jnp.int32, (seqs * res // SUBLANES, SUBLANES, LANES), 1)
    lane_at = lax.broadcasted_iota(jnp.int32, (seqs * res // SUBLANES, SUBLANES, LANES), 2)
    own = blocks_at * per_row + row_at // res == lane_at // pack

    def to_lanes(column):
        tall = jnp.where(own, column.reshape(seqs * res // SUBLANES, SUBLANES, 1), 0.0)
        tall = jnp.sum(tall, axis=0)
        total = tall[:res]
        for n in range(1, per_row):
            total = total + tall[n * res : (n + 1) * res]
        return total

    sums = spread(
        [
            jnp.broadcast_to(weight_sum[g * high : (g + 1) * high], (high, LANES))
            for g in range(pack)
        ]
    )
    mean_at, scale_at = to_lanes(mean), to_lanes(scale)
    for j in range(res):
        pieces = []
        for g in range(pack):
            piece = product[g * high : (g + 1) * high]
            shift = (g - j) % LANES
            pieces.append(pltpu.roll(piece, shift, 1) if shift else piece)
        total = (spread(pieces) - mean_at[j : j + 1] * sums) * scale_at[j : j + 1]
        tall[pl.ds(j, high, stride=res), :] = total
    right_own[...] = tall[...].astype(BF16)

    my_slot = lax.rem(my_res, half)
    away = lax.rem(my_seq - my_col + n_seq, n_seq)
    right_at = right_got.at[away * half + my_slot]

    def send_right(res_at):
        return pltpu.make_async_remote_copy(
            src_ref=right_own,
            dst_ref=right_at,
            send_sem=load_sem.at[0],
            recv_sem=rrecv_sem,
            device_id={"res": res_at, "seq": my_col},
            device_id_type=MESH,
        )

    def lower(res_at, carry):
        @pl.when(res_at < my_res)
        def _():
            send_right(res_at).start()

        return carry

    lax.fori_loop(0, n_res - 1, lower, 0, unroll=short)
    keep = pltpu.make_async_copy(right_own, right_at, rrecv_sem)

    @pl.when(away == 0)
    def _():
        keep.start()

    @pl.when(away != 0)
    def _():
        send_right(my_res).start()

    await_bytes(wl_ref, load_sem.at[n_seq])
    normed = (centred * scale * gain_ref[...]).astype(BF16)
    wl_wide = jnp.concatenate([wl_ref[...]] * pack, 0)
    left_own[...] = dot_last(normed, wl_wide).astype(BF16)
    await_bytes(late_bytes, load_sem.at[1])
    left_sends = []
    for k in range(1, n_seq):
        copy = pltpu.make_async_remote_copy(
            src_ref=left_own,
            dst_ref=left_got.at[n_seq - k - 1],
            send_sem=load_sem.at[k],
            recv_sem=lrecv_sem.at[n_seq - k - 1],
            device_id={"res": my_res, "seq": lax.rem(my_seq + k, n_seq)},
            device_id_type=MESH,
        )
        copy.start()
        left_sends.append(copy)

    wide_ref[...] = w_ref[...].astype(F32)
    for h in range(high):
        for g in range(pack):
            e = g * high + h
            at = (h // per_row * pack + g) * ch
            out_at = h % per_row * cz
            mixed_ref[at : at + ch, out_at : out_at + cz] = wide_ref[
                pl.ds(e, ch, stride=ch), :
            ].astype(BF16)

    to_row = lax.broadcasted_iota(jnp.int32, (res * LANES, seqs * res), 0)
    from_row = lax.broadcasted_iota(jnp.int32, (res * LANES, seqs * res), 1)
    picked = (to_row % LANES) // pack * res + to_row // LANES == from_row
    pick = picked.astype(F32).astype(BF16)
    group_at = lax.broadcasted_iota(jnp.int32, (LANES, pack * ch), 0) % pack
    copy_at = lax.broadcasted_iota(jnp.int32, (LANES, pack * ch), 1) // ch

    def place(part, source):
        for i in range(res):
            own_rows = pick[i * LANES : (i + 1) * LANES]
            blocks[part * LANES : (part + 1) * LANES, i * pack * ch : (i + 1) * pack * ch] = (
                jnp.where(group_at == copy_at, dot(own_rows, source), 0.0).astype(BF16)
            )

    place(0, left_own[...])
    for k in range(1, n_seq):
        left_sends[n_seq - k - 1].wait_recv()
        place(k, left_got[k - 1])

    for level in range(levels):
        above = jnp.minimum((level + 1) * step - 1 - my_res, step)

        @pl.when(above > 0)
        def _():
            pl.semaphore_wait(ready_sem.at[level], above)

            def higher(n, carry):
                @pl.when(level * step + n > my_res)
                def _():
                    send_right(level * step + n).start()

                return carry

            lax.fori_loop(0, step, higher, 0, unroll=short)

    await_bytes(right_got, rrecv_sem)
    group = math.gcd(half, 4)

    tiles = high // per_row

    def columns(n):
        got = jnp.concatenate(
            [
                jnp.concatenate(
                    [
                        right_got[
                            pl.ds(part * half + n * group, group),
                            tile * SUBLANES : (tile + 1) * SUBLANES,
                        ].reshape(group * SUBLANES, LANES)
                        for part in range(n_seq)
                    ],
                    1,
                )
                for tile in range(tiles)
            ],
            0,
        )
        outer = dot(got, blocks[...])
        count = group * SUBLANES
        lhs = jnp.concatenate(
            [
                jnp.concatenate(
                    [
                        outer[tile * count : (tile + 1) * count, i * LANES : (i + 1) * LANES]
                        for tile in range(tiles)
                    ],
                    1,
                )
                for i in range(res)
            ],
            0,
        ).astype(BF16)
        pairs = dot(lhs, mixed_ref[...])
        for i in range(res):
            for slot in range(0, group, per_row):
                pieces = []
                for q in range(per_row):
                    at = i * count + (slot + q) * SUBLANES
                    piece = pairs[at : at + res, :cz]
                    for h in range(1, per_row):
                        piece = piece + pairs[at + h * res : at + (h + 1) * res, h * cz : (h + 1) * cz]
                    pieces.append(piece)
                result = jnp.concatenate(pieces, 0) * inv_count + bias_ref[...]
                at = pl.ds(pl.multiple_of((n * group + slot) * res, SUBLANES), SUBLANES)
                out_ref[i, at, :] = result.astype(out_ref.dtype)

    if half == group:
        columns(0)
    else:

        @pl.loop(0, half // group)
        def _(n):
            columns(n)

    for copy in left_sends:
        copy.wait_send()

    @pl.when(away == 0)
    def _():
        await_bytes(right_got.at[pl.ds(0, n_res - 1)], load_sem.at[0])

    @pl.when(away != 0)
    def _():
        await_bytes(right_got, load_sem.at[0])


def scoped(n_res, n_seq, *refs):
    pl.run_scoped(
        functools.partial(kernel, n_res, n_seq, *refs),
        pltpu.SemaphoreType.DMA((n_seq + 1,)),
        pltpu.SemaphoreType.DMA((n_seq - 1,)),
        pltpu.SemaphoreType.DMA,
        pltpu.SemaphoreType.REGULAR((2 * n_seq,)),
    )


def on_device(alignment, ln_gain, proj_left, proj_right, out_weight, out_bias):
    n_res, n_seq = lax.axis_size("res"), lax.axis_size("seq")
    seqs, res, width = alignment.shape
    ch = proj_left.shape[1]
    cz = out_weight.shape[1]
    half = n_res // n_seq
    cols = res * half
    pack = LANES // seqs
    rows = res * (ch // pack)
    wide = res * pack * ch
    group = math.gcd(half, 4)
    per_row = SUBLANES // res
    unit = 2 * LANES * 4
    early = (seqs * res * width + ch * width) * 2 + width * 4
    late = ch * ch * cz * 2 + cz * 4
    return pl.pallas_call(
        functools.partial(scoped, n_res, n_seq),
        out_shape=pltpu.VMEM((res, cols, cz), BF16),
        in_specs=[pl.BlockSpec(memory_space=pl.ANY)] * 6,
        out_specs=pl.BlockSpec(memory_space=pltpu.VMEM),
        scratch_shapes=[
            pltpu.VMEM((seqs, res, width), BF16),
            pltpu.VMEM((1, width), F32),
            pltpu.VMEM((ch, width), BF16),
            pltpu.VMEM((ch, width), BF16),
            pltpu.VMEM((ch * ch, cz), BF16),
            pltpu.VMEM((1, cz), F32),
            pltpu.VMEM((ch * ch, cz), F32),
            pltpu.VMEM((ch * ch // per_row, per_row * cz), BF16),
            pltpu.VMEM((res * seqs, pack * ch), BF16),
            pltpu.VMEM((n_seq - 1, res * seqs, pack * ch), BF16),
            pltpu.VMEM((n_seq * LANES, wide), BF16),
            pltpu.VMEM((rows, LANES), BF16),
            pltpu.VMEM((n_res, rows, LANES), BF16),
            pltpu.VMEM((rows, LANES), F32),
            pltpu.VMEM((early // unit, 2, LANES), F32),
            pltpu.VMEM((late // (unit // 2), 1, LANES), F32),
        ],
        compiler_params=pltpu.CompilerParams(collective_id=0, has_side_effects=True),
    )(
        alignment,
        ln_gain.reshape(1, width),
        proj_left.T,
        proj_right.T,
        out_weight,
        out_bias.reshape(1, cz),
    )


def solution(mesh):
    placed = (P(("groups", "seq"), "res", None), P(), P(), P(), P(), P())
    return jax.shard_map(
        on_device,
        mesh=mesh,
        in_specs=placed,
        out_specs=P(("groups", "res"), "seq", None),
        check_vma=False,
    )
```

```python
import functools
import math

import jax
import jax.numpy as jnp
from jax import lax
from jax.experimental import pallas as pl
from jax.experimental.pallas import tpu as pltpu
from jax.sharding import PartitionSpec as P

F32 = jnp.float32
BF16 = jnp.bfloat16
MESH = pl.DeviceIdType.MESH
LANES = 128
SUBLANES = 8


def kernel(
    n_res, n_seq, x_hbm, gain_hbm, wl_hbm, wr_hbm, w_hbm, bias_hbm, out_ref,
    x_ref, gain_ref, wl_ref, wr_ref, w_ref, bias_ref,
    wide_ref, mixed_ref, left_own, left_got, blocks, right_own, right_got, tall,
    held, early_bytes, late_bytes, load_sem, lrecv_sem, rrecv_sem, ready_sem, *accs,
):
    seqs, res, width = x_ref.shape
    ch = wl_ref.shape[0]
    cz = bias_ref.shape[1]
    pack = LANES // seqs
    high = ch // pack
    half = n_res // n_seq
    rows = res * high
    inv_count = 1.0 / (seqs * n_seq)
    my_res, my_seq = lax.axis_index("res"), lax.axis_index("seq")
    my_col = my_res // half
    first = my_seq * half
    short = n_res <= 8
    levels = ready_sem.shape[0]
    group = math.gcd(half, 4)
    chunks = (len(accs) // 2 - 2) // 2
    step = n_res // levels

    def load(src, dst, n):
        copy = pltpu.make_async_copy(src, dst, load_sem.at[n])
        copy.start()

    def await_bytes(ref, sem):
        pltpu.make_async_copy(ref, ref, sem).wait()

    for n in range(4):
        at = pl.ds(n * (seqs // 4), seqs // 4)
        load(x_hbm.at[at], x_ref.at[at], 0)
    load(wr_hbm, wr_ref, 0)
    load(gain_hbm, gain_ref, 0)
    load(wl_hbm, wl_ref, n_seq)
    load(w_hbm, w_ref, 1)
    load(bias_hbm, bias_ref, 1)

    barrier = pltpu.get_barrier_semaphore()

    def signal(sem, res_at, seq_at):
        pl.semaphore_signal(
            sem, inc=1, device_id={"res": res_at, "seq": seq_at}, device_id_type=MESH
        )

    for k in range(1, n_seq):
        signal(barrier, my_res, lax.rem(my_seq + k, n_seq))

    def greet(res_at, carry):
        for seq_at in range(n_seq):

            @pl.when((res_at > my_res) & ((my_col == seq_at) | (res_at // half == my_seq)))
            def _():
                signal(barrier, res_at, seq_at)

        return carry

    lax.fori_loop(0, n_res, greet, 0, unroll=short)
    near = jnp.minimum(jnp.maximum(my_res - first, 0), half)
    pl.semaphore_wait(barrier, my_res + (n_seq - 1) * near + n_seq - 1)

    my_level = my_res // step

    def answer(n, carry):
        for seq_at in range(n_seq):

            @pl.when(first + n < my_res)
            def _():
                signal(ready_sem.at[my_level], first + n, seq_at)

        return carry

    lax.fori_loop(0, half, answer, 0, unroll=short)

    await_bytes(early_bytes, load_sem.at[0])

    values = x_ref[...].astype(F32).reshape(seqs * res, width)
    side_acc, row_acc, first_acc, second_acc = [
        [accs[q * len(accs) // 2 + n] for q in range(2)] for n in range(2)
    ] + [[accs[q * len(accs) // 2 + 2 + k * chunks : ][:chunks] for q in range(2)] for k in range(2)]
    gained = (wr_ref[...].astype(F32) * gain_ref[...]).astype(BF16)
    octets = values.reshape(seqs * res // SUBLANES, SUBLANES, width)

    def repeated(j):
        parts = [
            jnp.broadcast_to(octets[:, n * res + j : n * res + j + 1], (octets.shape[0], res, width))
            for n in range(SUBLANES // res)
        ]
        return jnp.concatenate(parts, 1).reshape(seqs * res, width).astype(BF16)

    for q in range(2):
        pltpu.matmul_push_rhs(
            jnp.concatenate([repeated(q * res // 2 + n) for n in range(res // 2)], 0),
            0,
            q,
            transpose=True,
        )
        pltpu.matmul_acc_lhs(side_acc[q], gained, load_staged_rhs=0)
    product = [pltpu.matmul_pop(side_acc[q]) for q in range(2)]
    weight_sum = jnp.sum(gained.astype(F32), axis=-1, keepdims=True)
    mean = jnp.mean(values, axis=-1, keepdims=True)
    centred = values - mean
    variance = jnp.mean(centred * centred, axis=-1, keepdims=True)
    scale = lax.rsqrt(variance + 1e-05)

    lane = lax.broadcasted_iota(jnp.int32, (high, LANES), 1)
    in_group = [lane % pack == g for g in range(pack)]

    def spread(pieces):
        total = pieces[0]
        for g in range(1, pack):
            total = jnp.where(in_group[g], pieces[g], total)
        return total

    per_row = SUBLANES // res
    blocks_at = lax.broadcasted_iota(jnp.int32, (seqs * res // SUBLANES, SUBLANES, LANES), 0)
    row_at = lax.broadcasted_iota(jnp.int32, (seqs * res // SUBLANES, SUBLANES, LANES), 1)
    lane_at = lax.broadcasted_iota(jnp.int32, (seqs * res // SUBLANES, SUBLANES, LANES), 2)
    own = blocks_at * per_row + row_at // res == lane_at // pack

    def to_lanes(column):
        tall = jnp.where(own, column.reshape(seqs * res // SUBLANES, SUBLANES, 1), 0.0)
        tall = jnp.sum(tall, axis=0)
        total = tall[:res]
        for n in range(1, per_row):
            total = total + tall[n * res : (n + 1) * res]
        return total

    sums = spread(
        [
            jnp.broadcast_to(weight_sum[g * high : (g + 1) * high], (high, LANES))
            for g in range(pack)
        ]
    )
    mean_at, scale_at = to_lanes(mean), to_lanes(scale)
    for j in range(res):
        at = j % (res // 2) * LANES
        pieces = [
            product[j * 2 // res][g * high : (g + 1) * high, at : at + LANES] for g in range(pack)
        ]
        total = (spread(pieces) - mean_at[j : j + 1] * sums) * scale_at[j : j + 1]
        tall[pl.ds(j, high, stride=res), :] = total
    right_own[...] = tall[...].astype(BF16)

    my_slot = lax.rem(my_res, half)
    away = lax.rem(my_seq - my_col + n_seq, n_seq)

    def last_slot(res_at):
        return jnp.where(res_at < n_res - half, half - 1, min(1, half - 1))

    def comes_last(res_at):
        return (my_seq == 0) & (my_slot == last_slot(res_at))

    def right_at(res_at):
        return right_got.at[jnp.where(comes_last(res_at), n_res, away * half + my_slot)]

    def right_sem(res_at):
        return rrecv_sem.at[jnp.where(comes_last(res_at), 1, 0)]

    def send_right(res_at):
        return pltpu.make_async_remote_copy(
            src_ref=right_own,
            dst_ref=right_at(res_at),
            send_sem=load_sem.at[0],
            recv_sem=right_sem(res_at),
            device_id={"res": res_at, "seq": my_col},
            device_id_type=MESH,
        )

    def lower(res_at, carry):
        @pl.when(res_at < my_res)
        def _():
            send_right(res_at).start()

        return carry

    lax.fori_loop(0, n_res - 1, lower, 0, unroll=short)
    keep = pltpu.make_async_copy(right_own, right_at(my_res), right_sem(my_res))

    @pl.when(away == 0)
    def _():
        keep.start()

    @pl.when(away != 0)
    def _():
        send_right(my_res).start()

    await_bytes(wl_ref, load_sem.at[n_seq])
    normed = (centred * scale * gain_ref[...]).astype(BF16)
    pltpu.matmul_push_rhs(jnp.concatenate([wl_ref[...]] * (width // ch), 0), 0, 0, transpose=True)
    pltpu.matmul_acc_lhs(row_acc[0], normed, load_staged_rhs=0)
    left_own[...] = pltpu.matmul_pop(row_acc[0])[:, : pack * ch].astype(BF16)
    last = lax.rem(n_seq - my_seq, n_seq) * half + last_slot(my_res)
    right_got[last] = jnp.zeros((rows, LANES), BF16)
    await_bytes(late_bytes, load_sem.at[1])
    left_sends = []
    for k in range(1, n_seq):
        copy = pltpu.make_async_remote_copy(
            src_ref=left_own,
            dst_ref=left_got.at[n_seq - k - 1],
            send_sem=load_sem.at[k],
            recv_sem=lrecv_sem.at[n_seq - k - 1],
            device_id={"res": my_res, "seq": lax.rem(my_seq + k, n_seq)},
            device_id_type=MESH,
        )
        copy.start()
        left_sends.append(copy)

    wide_ref[...] = w_ref[...].astype(F32)
    for h in range(high):
        for g in range(pack):
            e = g * high + h
            at = (h // per_row * pack + g) * ch
            out_at = h % per_row * cz
            mixed_ref[at : at + ch, out_at : out_at + cz] = wide_ref[
                pl.ds(e, ch, stride=ch), :
            ].astype(BF16)

    for k in range(1, n_seq):
        left_sends[n_seq - k - 1].wait_recv()
    sides = jnp.concatenate([left_own[...]] + [left_got[k - 1] for k in range(1, n_seq)], 0)
    to_row = lax.broadcasted_iota(jnp.int32, (LANES, n_seq * LANES), 0)
    from_row = lax.broadcasted_iota(jnp.int32, (LANES, n_seq * LANES), 1)
    offset = from_row - to_row // pack * res
    copy_at = lax.broadcasted_iota(jnp.int32, (LANES, pack * ch), 1) // ch
    group_at = lax.broadcasted_iota(jnp.int32, (LANES, pack * ch), 0) % pack
    for q in range(2):
        pltpu.matmul_push_rhs(jnp.concatenate([sides] * 2, 1), 0, q)
    for part in range(n_seq):
        for i in range(res):
            q = i % 2
            pick = (offset == part * LANES + i).astype(F32).astype(BF16)
            pltpu.matmul_acc_lhs(
                row_acc[q], pick, load_staged_rhs=0 if part == 0 and i < 2 else None
            )
            block = pltpu.matmul_pop(row_acc[q])[:, : pack * ch]
            blocks[part * LANES : (part + 1) * LANES, i * pack * ch : (i + 1) * pack * ch] = (
                jnp.where(group_at == copy_at, block, 0.0).astype(BF16)
            )

    for level in range(levels):
        above = jnp.minimum((level + 1) * step - 1 - my_res, step)

        @pl.when(above > 0)
        def _():
            pl.semaphore_wait(ready_sem.at[level], above)

            def higher(n, carry):
                @pl.when(level * step + n > my_res)
                def _():
                    send_right(level * step + n).start()

                return carry

            lax.fori_loop(0, step, higher, 0, unroll=short)

    tiles = high // per_row
    wide = 2 * LANES

    def push_weights():
        for q in range(2):
            pltpu.matmul_push_rhs(blocks[:, q * wide : (q + 1) * wide], 0, q)
            pltpu.matmul_push_rhs(mixed_ref[q * wide : (q + 1) * wide, :], 1, q)

    def first_matmul(n, lhs):
        for q in range(2):
            pltpu.matmul_acc_lhs(first_acc[q][n], lhs, load_staged_rhs=None if n else 0)

    def second_matmul(n, lhs):
        for q in range(2):
            pltpu.matmul_acc_lhs(second_acc[q][n], lhs[q], load_staged_rhs=None if n else 1)

    def second_result(n):
        both = pltpu.matmul_pop(second_acc[0][n]) + pltpu.matmul_pop(second_acc[1][n])
        found = []
        for at in range(0, 2 * SUBLANES, SUBLANES):
            piece = both[at : at + res, :cz]
            for h in range(1, per_row):
                piece = piece + both[at + h * res : at + (h + 1) * res, h * cz : (h + 1) * cz]
            found.append(piece)
        return found

    def lanes_of(outer, i):
        return outer[i // 2][:, i % 2 * LANES : (i % 2 + 1) * LANES]

    def columns(n):
        pairs = range(group // 2)
        for pair in pairs:
            for tile in range(tiles):
                lhs = [
                    right_got[
                        pl.ds(part * half + n * group + 2 * pair, 2),
                        tile * SUBLANES : (tile + 1) * SUBLANES,
                    ].reshape(2 * SUBLANES, LANES)
                    for part in range(n_seq)
                ]
                first_matmul(pair * tiles + tile, jnp.concatenate(lhs, 1))
        outer = [
            [pltpu.matmul_pop(first_acc[q][k]) for q in range(2)] for k in range(len(pairs) * tiles)
        ]
        for pair in pairs:
            for i in range(res):
                lhs = [
                    jnp.concatenate(
                        [
                            lanes_of(outer[pair * tiles + 2 * q + tile], i).astype(BF16)
                            for tile in range(tiles // 2)
                        ],
                        1,
                    )
                    for q in range(2)
                ]
                second_matmul(pair * res + i, lhs)
        for pair in pairs:
            for i in range(res):
                found = second_result(pair * res + i)
                at = pl.ds(pl.multiple_of((n * group + 2 * pair) * res, SUBLANES), SUBLANES)
                held[i, at, :] = jnp.concatenate(found, 0) * inv_count + bias_ref[...]

    if half == group:
        push_weights()
        await_bytes(right_got.at[pl.ds(0, n_res - 1)], rrecv_sem.at[0])
        columns(0)
    else:
        await_bytes(right_got.at[pl.ds(0, n_res - 1)], rrecv_sem.at[0])

        @pl.loop(0, half // group)
        def _(n):
            push_weights()
            columns(n)

    push_weights()
    my_last = last_slot(my_res)
    my_part = lax.rem(n_seq - my_seq, n_seq)
    await_bytes(right_got.at[n_res], rrecv_sem.at[1])
    for pair in range(tiles // 2):
        block = right_got[n_res, pair * 2 * SUBLANES : (pair + 1) * 2 * SUBLANES, :]
        zero = jnp.zeros_like(block)
        lhs = [jnp.where(my_part == part, block, zero) for part in range(n_seq)]
        first_matmul(pair, jnp.concatenate(lhs, 1))
    outer = [[pltpu.matmul_pop(first_acc[q][k]) for q in range(2)] for k in range(tiles // 2)]
    for pair in range(res // 2):
        lhs = []
        for q in range(2):
            pieces = []
            for tile in range(tiles // 2):
                at = slice(tile * SUBLANES, (tile + 1) * SUBLANES)
                pieces.append(
                    jnp.concatenate(
                        [lanes_of(outer[q], 2 * pair + k)[at] for k in range(2)], 0
                    ).astype(BF16)
                )
            lhs.append(jnp.concatenate(pieces, 1))
        second_matmul(pair, lhs)
    found = [piece for pair in range(res // 2) for piece in second_result(pair)]

    def finish(n):
        for i in range(res):
            piece = found[i] * inv_count
            for pair in range(group // 2):
                slot = n * group + 2 * pair
                at = pl.ds(pl.multiple_of(slot * res, SUBLANES), SUBLANES)
                added = [jnp.where(my_last == slot + k, piece, 0.0) for k in range(2)]
                out_ref[i, at, :] = (held[i, at, :] + jnp.concatenate(added, 0)).astype(BF16)

    if half == group:
        finish(0)
    else:

        @pl.loop(0, half // group)
        def _(n):
            finish(n)

    for copy in left_sends:
        copy.wait_send()

    @pl.when(away == 0)
    def _():
        await_bytes(right_got.at[pl.ds(0, n_res - 1)], load_sem.at[0])

    @pl.when(away != 0)
    def _():
        await_bytes(right_got.at[pl.ds(0, n_res)], load_sem.at[0])


def scoped(n_res, n_seq, *refs):
    accumulators = [
        pltpu.ACC(q)((m, 2 * LANES), F32) for q in range(2) for m in [32, LANES] + [16] * 16
    ]
    pl.run_scoped(
        functools.partial(kernel, n_res, n_seq, *refs),
        pltpu.SemaphoreType.DMA((n_seq + 1,)),
        pltpu.SemaphoreType.DMA((n_seq - 1,)),
        pltpu.SemaphoreType.DMA((2,)),
        pltpu.SemaphoreType.REGULAR((2 * n_seq,)),
        *accumulators,
    )


def on_device(alignment, ln_gain, proj_left, proj_right, out_weight, out_bias):
    n_res, n_seq = lax.axis_size("res"), lax.axis_size("seq")
    seqs, res, width = alignment.shape
    ch = proj_left.shape[1]
    cz = out_weight.shape[1]
    half = n_res // n_seq
    cols = res * half
    pack = LANES // seqs
    rows = res * (ch // pack)
    wide = res * pack * ch
    group = math.gcd(half, 4)
    per_row = SUBLANES // res
    unit = 2 * LANES * 4
    early = (seqs * res * width + ch * width) * 2 + width * 4
    late = ch * ch * cz * 2 + cz * 4
    return pl.pallas_call(
        functools.partial(scoped, n_res, n_seq),
        out_shape=pltpu.VMEM((res, cols, cz), BF16),
        in_specs=[pl.BlockSpec(memory_space=pl.ANY)] * 6,
        out_specs=pl.BlockSpec(memory_space=pltpu.VMEM),
        scratch_shapes=[
            pltpu.VMEM((seqs, res, width), BF16),
            pltpu.VMEM((1, width), F32),
            pltpu.VMEM((ch, width), BF16),
            pltpu.VMEM((ch, width), BF16),
            pltpu.VMEM((ch * ch, cz), BF16),
            pltpu.VMEM((1, cz), F32),
            pltpu.VMEM((ch * ch, cz), F32),
            pltpu.VMEM((ch * ch // per_row, per_row * cz), BF16),
            pltpu.VMEM((res * seqs, pack * ch), BF16),
            pltpu.VMEM((n_seq - 1, res * seqs, pack * ch), BF16),
            pltpu.VMEM((n_seq * LANES, wide), BF16),
            pltpu.VMEM((rows, LANES), BF16),
            pltpu.VMEM((n_res + 1, rows, LANES), BF16),
            pltpu.VMEM((rows, LANES), F32),
            pltpu.VMEM((res, cols, cz), F32),
            pltpu.VMEM((early // unit, 2, LANES), F32),
            pltpu.VMEM((late // (unit // 2), 1, LANES), F32),
        ],
        compiler_params=pltpu.CompilerParams(collective_id=0, has_side_effects=True),
    )(
        alignment,
        ln_gain.reshape(1, width),
        proj_left.T,
        proj_right.T,
        out_weight,
        out_bias.reshape(1, cz),
    )


def solution(mesh):
    placed = (P(("groups", "seq"), "res", None), P(), P(), P(), P(), P())
    return jax.shard_map(
        on_device,
        mesh=mesh,
        in_specs=placed,
        out_specs=P(("groups", "res"), "seq", None),
        check_vma=False,
    )
```

```python
import functools
import math

import jax
import jax.numpy as jnp
from jax import lax
from jax.experimental import pallas as pl
from jax.experimental.pallas import tpu as pltpu
from jax.sharding import PartitionSpec as P

F32 = jnp.float32
BF16 = jnp.bfloat16
MESH = pl.DeviceIdType.MESH
LANES = 128
SUBLANES = 8


def kernel(
    n_res, n_seq, x_hbm, gain_hbm, wl_hbm, wr_hbm, w_hbm, bias_hbm, out_ref,
    x_ref, gain_ref, wl_ref, wr_ref, w_ref, bias_ref,
    wide_ref, mixed_ref, left_own, left_got, blocks, right_own, right_got, tall,
    held, early_bytes, late_bytes, load_sem, lrecv_sem, rrecv_sem, ready_sem, *accs,
):
    seqs, res, width = x_ref.shape
    ch = wl_ref.shape[0]
    cz = bias_ref.shape[1]
    pack = LANES // seqs
    high = ch // pack
    half = n_res // n_seq
    rows = res * high
    inv_count = 1.0 / (seqs * n_seq)
    my_res, my_seq = lax.axis_index("res"), lax.axis_index("seq")
    my_col = my_res // half
    first = my_seq * half
    short = n_res <= 8
    levels = ready_sem.shape[0]
    group = math.gcd(half, 4)
    chunks = (len(accs) // 2 - 2) // 2
    step = n_res // levels

    def load(src, dst, n):
        copy = pltpu.make_async_copy(src, dst, load_sem.at[n])
        copy.start()

    def await_bytes(ref, sem):
        pltpu.make_async_copy(ref, ref, sem).wait()

    for n in range(4):
        at = pl.ds(n * (seqs // 4), seqs // 4)
        load(x_hbm.at[at], x_ref.at[at], 0)
    load(wr_hbm, wr_ref, 0)
    load(gain_hbm, gain_ref, 0)
    load(wl_hbm, wl_ref, n_seq)
    load(w_hbm, w_ref, 1)
    load(bias_hbm, bias_ref, 1)

    barrier = pltpu.get_barrier_semaphore()

    def signal(sem, res_at, seq_at):
        pl.semaphore_signal(
            sem, inc=1, device_id={"res": res_at, "seq": seq_at}, device_id_type=MESH
        )

    for k in range(1, n_seq):
        signal(barrier, my_res, lax.rem(my_seq + k, n_seq))

    def greet(res_at, carry):
        for seq_at in range(n_seq):

            @pl.when((res_at > my_res) & ((my_col == seq_at) | (res_at // half == my_seq)))
            def _():
                signal(barrier, res_at, seq_at)

        return carry

    lax.fori_loop(0, n_res, greet, 0, unroll=short)
    def meet():
        near = jnp.minimum(jnp.maximum(my_res - first, 0), half)
        pl.semaphore_wait(barrier, my_res + (n_seq - 1) * near + n_seq - 1)

        my_level = my_res // step

        def answer(n, carry):
            for seq_at in range(n_seq):

                @pl.when(first + n < my_res)
                def _():
                    signal(ready_sem.at[my_level], first + n, seq_at)

            return carry

        lax.fori_loop(0, half, answer, 0, unroll=short)

    pl.when(my_res % 2 == 1)(meet)

    await_bytes(early_bytes, load_sem.at[0])

    values = x_ref[...].astype(F32).reshape(seqs * res, width)
    side_acc, row_acc, first_acc, second_acc = [
        [accs[q * len(accs) // 2 + n] for q in range(2)] for n in range(2)
    ] + [[accs[q * len(accs) // 2 + 2 + k * chunks : ][:chunks] for q in range(2)] for k in range(2)]
    gained = (wr_ref[...].astype(F32) * gain_ref[...]).astype(BF16)
    sublane = lax.broadcasted_iota(jnp.int32, (SUBLANES, LANES), 0)

    def repeated(j):
        source = sublane // res * res + j
        return jnp.concatenate(
            [
                jnp.concatenate(
                    [
                        jnp.take_along_axis(
                            values[at : at + SUBLANES, n * LANES : (n + 1) * LANES], source, 0
                        )
                        for n in range(width // LANES)
                    ],
                    1,
                )
                for at in range(0, seqs * res, SUBLANES)
            ],
            0,
        ).astype(BF16)

    for q in range(2):
        pltpu.matmul_push_rhs(
            jnp.concatenate([repeated(q * res // 2 + n) for n in range(res // 2)], 0),
            0,
            q,
            transpose=True,
        )
        pltpu.matmul_acc_lhs(side_acc[q], gained, load_staged_rhs=0)
    product = [pltpu.matmul_pop(side_acc[q]) for q in range(2)]
    weight_sum = jnp.sum(gained.astype(F32), axis=-1, keepdims=True)
    mean = jnp.mean(values, axis=-1, keepdims=True)
    centred = values - mean
    variance = jnp.mean(centred * centred, axis=-1, keepdims=True)
    scale = lax.rsqrt(variance + 1e-05)

    lane = lax.broadcasted_iota(jnp.int32, (high, LANES), 1)
    in_group = [lane % pack == g for g in range(pack)]

    def spread(pieces):
        total = pieces[0]
        for g in range(1, pack):
            total = jnp.where(in_group[g], pieces[g], total)
        return total

    per_row = SUBLANES // res
    blocks_at = lax.broadcasted_iota(jnp.int32, (seqs * res // SUBLANES, SUBLANES, LANES), 0)
    row_at = lax.broadcasted_iota(jnp.int32, (seqs * res // SUBLANES, SUBLANES, LANES), 1)
    lane_at = lax.broadcasted_iota(jnp.int32, (seqs * res // SUBLANES, SUBLANES, LANES), 2)
    own = blocks_at * per_row + row_at // res == lane_at // pack

    def to_lanes(column):
        tall = jnp.where(own, column.reshape(seqs * res // SUBLANES, SUBLANES, 1), 0.0)
        tall = jnp.sum(tall, axis=0)
        total = tall[:res]
        for n in range(1, per_row):
            total = total + tall[n * res : (n + 1) * res]
        return total

    sums = spread(
        [
            jnp.broadcast_to(weight_sum[g * high : (g + 1) * high], (high, LANES))
            for g in range(pack)
        ]
    )
    mean_at, scale_at = to_lanes(mean), to_lanes(scale)
    for j in range(res):
        at = j % (res // 2) * LANES
        pieces = [
            product[j * 2 // res][g * high : (g + 1) * high, at : at + LANES] for g in range(pack)
        ]
        total = (spread(pieces) - mean_at[j : j + 1] * sums) * scale_at[j : j + 1]
        tall[pl.ds(j, high, stride=res), :] = total
    right_own[...] = tall[...].astype(BF16)

    my_slot = lax.rem(my_res, half)
    away = lax.rem(my_seq - my_col + n_seq, n_seq)

    def last_slot(res_at):
        return jnp.where(res_at < n_res - half, half - 1, min(1, half - 1))

    def comes_last(res_at):
        return (my_seq == 0) & (my_slot == last_slot(res_at))

    def right_at(res_at):
        return right_got.at[jnp.where(comes_last(res_at), n_res, away * half + my_slot)]

    def right_sem(res_at):
        return rrecv_sem.at[jnp.where(comes_last(res_at), 1, 0)]

    def send_right(res_at):
        return pltpu.make_async_remote_copy(
            src_ref=right_own,
            dst_ref=right_at(res_at),
            send_sem=load_sem.at[0],
            recv_sem=right_sem(res_at),
            device_id={"res": res_at, "seq": my_col},
            device_id_type=MESH,
        )

    def lower(res_at, carry):
        @pl.when(res_at < my_res)
        def _():
            send_right(res_at).start()

        return carry

    pl.when(my_res % 2 == 0)(meet)
    lax.fori_loop(0, n_res - 1, lower, 0, unroll=short)
    keep = pltpu.make_async_copy(right_own, right_at(my_res), right_sem(my_res))

    @pl.when(away == 0)
    def _():
        keep.start()

    @pl.when(away != 0)
    def _():
        send_right(my_res).start()

    await_bytes(wl_ref, load_sem.at[n_seq])
    normed = (centred * scale * gain_ref[...]).astype(BF16)
    pltpu.matmul_push_rhs(jnp.concatenate([wl_ref[...]] * (width // ch), 0), 0, 0, transpose=True)
    pltpu.matmul_acc_lhs(row_acc[0], normed, load_staged_rhs=0)
    left_own[...] = pltpu.matmul_pop(row_acc[0])[:, : pack * ch].astype(BF16)
    last = lax.rem(n_seq - my_seq, n_seq) * half + last_slot(my_res)
    right_got[last] = jnp.zeros((rows, LANES), BF16)
    await_bytes(late_bytes, load_sem.at[1])
    left_sends = []
    for k in range(1, n_seq):
        copy = pltpu.make_async_remote_copy(
            src_ref=left_own,
            dst_ref=left_got.at[n_seq - k - 1],
            send_sem=load_sem.at[k],
            recv_sem=lrecv_sem.at[n_seq - k - 1],
            device_id={"res": my_res, "seq": lax.rem(my_seq + k, n_seq)},
            device_id_type=MESH,
        )
        copy.start()
        left_sends.append(copy)

    wide_ref[...] = w_ref[...].astype(F32)
    for h in range(high):
        for g in range(pack):
            e = g * high + h
            at = (h // per_row * pack + g) * ch
            out_at = h % per_row * cz
            mixed_ref[at : at + ch, out_at : out_at + cz] = wide_ref[
                pl.ds(e, ch, stride=ch), :
            ].astype(BF16)

    for k in range(1, n_seq):
        left_sends[n_seq - k - 1].wait_recv()
    sides = jnp.concatenate([left_own[...]] + [left_got[k - 1] for k in range(1, n_seq)], 0)
    to_row = lax.broadcasted_iota(jnp.int32, (LANES, n_seq * LANES), 0)
    from_row = lax.broadcasted_iota(jnp.int32, (LANES, n_seq * LANES), 1)
    offset = from_row - to_row // pack * res
    copy_at = lax.broadcasted_iota(jnp.int32, (LANES, pack * ch), 1) // ch
    group_at = lax.broadcasted_iota(jnp.int32, (LANES, pack * ch), 0) % pack
    for q in range(2):
        pltpu.matmul_push_rhs(jnp.concatenate([sides] * 2, 1), 0, q)
    for part in range(n_seq):
        for i in range(res):
            q = i % 2
            pick = (offset == part * LANES + i).astype(F32).astype(BF16)
            pltpu.matmul_acc_lhs(
                row_acc[q], pick, load_staged_rhs=0 if part == 0 and i < 2 else None
            )
            block = pltpu.matmul_pop(row_acc[q])[:, : pack * ch]
            blocks[part * LANES : (part + 1) * LANES, i * pack * ch : (i + 1) * pack * ch] = (
                jnp.where(group_at == copy_at, block, 0.0).astype(BF16)
            )

    for level in range(levels):
        above = jnp.minimum((level + 1) * step - 1 - my_res, step)

        @pl.when(above > 0)
        def _():
            pl.semaphore_wait(ready_sem.at[level], above)

            def higher(n, carry):
                @pl.when(level * step + n > my_res)
                def _():
                    send_right(level * step + n).start()

                return carry

            lax.fori_loop(0, step, higher, 0, unroll=short)

    tiles = high // per_row
    wide = 2 * LANES

    def push_weights():
        for q in range(2):
            pltpu.matmul_push_rhs(blocks[:, q * wide : (q + 1) * wide], 0, q)
            pltpu.matmul_push_rhs(mixed_ref[q * wide : (q + 1) * wide, :], 1, q)

    def first_matmul(n, lhs):
        for q in range(2):
            pltpu.matmul_acc_lhs(first_acc[q][n], lhs, load_staged_rhs=None if n else 0)

    def second_matmul(n, lhs):
        for q in range(2):
            pltpu.matmul_acc_lhs(second_acc[q][n], lhs[q], load_staged_rhs=None if n else 1)

    def second_result(n):
        both = pltpu.matmul_pop(second_acc[0][n]) + pltpu.matmul_pop(second_acc[1][n])
        found = []
        for at in range(0, 2 * SUBLANES, SUBLANES):
            piece = both[at : at + res, :cz]
            for h in range(1, per_row):
                piece = piece + both[at + h * res : at + (h + 1) * res, h * cz : (h + 1) * cz]
            found.append(piece)
        return found

    def lanes_of(outer, i):
        return outer[i // 2][:, i % 2 * LANES : (i % 2 + 1) * LANES]

    def columns(n):
        pairs = range(group // 2)
        for pair in pairs:
            for tile in range(tiles):
                lhs = [
                    right_got[
                        pl.ds(part * half + n * group + 2 * pair, 2),
                        tile * SUBLANES : (tile + 1) * SUBLANES,
                    ].reshape(2 * SUBLANES, LANES)
                    for part in range(n_seq)
                ]
                first_matmul(pair * tiles + tile, jnp.concatenate(lhs, 1))
        outer = [
            [pltpu.matmul_pop(first_acc[q][k]) for q in range(2)] for k in range(len(pairs) * tiles)
        ]
        for pair in pairs:
            for i in range(res):
                lhs = [
                    jnp.concatenate(
                        [
                            lanes_of(outer[pair * tiles + 2 * q + tile], i).astype(BF16)
                            for tile in range(tiles // 2)
                        ],
                        1,
                    )
                    for q in range(2)
                ]
                second_matmul(pair * res + i, lhs)
        for pair in pairs:
            for i in range(res):
                found = second_result(pair * res + i)
                at = pl.ds(pl.multiple_of((n * group + 2 * pair) * res, SUBLANES), SUBLANES)
                held[i, at, :] = jnp.concatenate(found, 0) * inv_count + bias_ref[...]

    if half == group:
        push_weights()
        await_bytes(right_got.at[pl.ds(0, n_res - 1)], rrecv_sem.at[0])
        columns(0)
    else:
        await_bytes(right_got.at[pl.ds(0, n_res - 1)], rrecv_sem.at[0])

        @pl.loop(0, half // group)
        def _(n):
            push_weights()
            columns(n)

    push_weights()
    my_last = last_slot(my_res)
    my_part = lax.rem(n_seq - my_seq, n_seq)
    await_bytes(right_got.at[n_res], rrecv_sem.at[1])
    for pair in range(tiles // 2):
        block = right_got[n_res, pair * 2 * SUBLANES : (pair + 1) * 2 * SUBLANES, :]
        zero = jnp.zeros_like(block)
        lhs = [jnp.where(my_part == part, block, zero) for part in range(n_seq)]
        first_matmul(pair, jnp.concatenate(lhs, 1))
    outer = [[pltpu.matmul_pop(first_acc[q][k]) for q in range(2)] for k in range(tiles // 2)]
    for pair in range(res // 2):
        lhs = []
        for q in range(2):
            pieces = []
            for tile in range(tiles // 2):
                at = slice(tile * SUBLANES, (tile + 1) * SUBLANES)
                pieces.append(
                    jnp.concatenate(
                        [lanes_of(outer[q], 2 * pair + k)[at] for k in range(2)], 0
                    ).astype(BF16)
                )
            lhs.append(jnp.concatenate(pieces, 1))
        second_matmul(pair, lhs)
    found = [piece for pair in range(res // 2) for piece in second_result(pair)]

    def finish(n):
        for i in range(res):
            piece = found[i] * inv_count
            for pair in range(group // 2):
                slot = n * group + 2 * pair
                at = pl.ds(pl.multiple_of(slot * res, SUBLANES), SUBLANES)
                added = [jnp.where(my_last == slot + k, piece, 0.0) for k in range(2)]
                out_ref[i, at, :] = (held[i, at, :] + jnp.concatenate(added, 0)).astype(BF16)

    if half == group:
        finish(0)
    else:

        @pl.loop(0, half // group)
        def _(n):
            finish(n)

    for copy in left_sends:
        copy.wait_send()

    @pl.when(away == 0)
    def _():
        await_bytes(right_got.at[pl.ds(0, n_res - 1)], load_sem.at[0])

    @pl.when(away != 0)
    def _():
        await_bytes(right_got.at[pl.ds(0, n_res)], load_sem.at[0])


def scoped(n_res, n_seq, *refs):
    accumulators = [
        pltpu.ACC(q)((m, 2 * LANES), F32) for q in range(2) for m in [32, LANES] + [16] * 16
    ]
    pl.run_scoped(
        functools.partial(kernel, n_res, n_seq, *refs),
        pltpu.SemaphoreType.DMA((n_seq + 1,)),
        pltpu.SemaphoreType.DMA((n_seq - 1,)),
        pltpu.SemaphoreType.DMA((2,)),
        pltpu.SemaphoreType.REGULAR((2 * n_seq,)),
        *accumulators,
    )


def on_device(alignment, ln_gain, proj_left, proj_right, out_weight, out_bias):
    n_res, n_seq = lax.axis_size("res"), lax.axis_size("seq")
    seqs, res, width = alignment.shape
    ch = proj_left.shape[1]
    cz = out_weight.shape[1]
    half = n_res // n_seq
    cols = res * half
    pack = LANES // seqs
    rows = res * (ch // pack)
    wide = res * pack * ch
    group = math.gcd(half, 4)
    per_row = SUBLANES // res
    unit = 2 * LANES * 4
    early = (seqs * res * width + ch * width) * 2 + width * 4
    late = ch * ch * cz * 2 + cz * 4
    return pl.pallas_call(
        functools.partial(scoped, n_res, n_seq),
        out_shape=pltpu.VMEM((res, cols, cz), BF16),
        in_specs=[pl.BlockSpec(memory_space=pl.ANY)] * 6,
        out_specs=pl.BlockSpec(memory_space=pltpu.VMEM),
        scratch_shapes=[
            pltpu.VMEM((seqs, res, width), BF16),
            pltpu.VMEM((1, width), F32),
            pltpu.VMEM((ch, width), BF16),
            pltpu.VMEM((ch, width), BF16),
            pltpu.VMEM((ch * ch, cz), BF16),
            pltpu.VMEM((1, cz), F32),
            pltpu.VMEM((ch * ch, cz), F32),
            pltpu.VMEM((ch * ch // per_row, per_row * cz), BF16),
            pltpu.VMEM((res * seqs, pack * ch), BF16),
            pltpu.VMEM((n_seq - 1, res * seqs, pack * ch), BF16),
            pltpu.VMEM((n_seq * LANES, wide), BF16),
            pltpu.VMEM((rows, LANES), BF16),
            pltpu.VMEM((n_res + 1, rows, LANES), BF16),
            pltpu.VMEM((rows, LANES), F32),
            pltpu.VMEM((res, cols, cz), F32),
            pltpu.VMEM((early // unit, 2, LANES), F32),
            pltpu.VMEM((late // (unit // 2), 1, LANES), F32),
        ],
        compiler_params=pltpu.CompilerParams(collective_id=0, has_side_effects=True),
    )(
        alignment,
        ln_gain.reshape(1, width),
        proj_left.T,
        proj_right.T,
        out_weight,
        out_bias.reshape(1, cz),
    )


def solution(mesh):
    placed = (P(("groups", "seq"), "res", None), P(), P(), P(), P(), P())
    return jax.shard_map(
        on_device,
        mesh=mesh,
        in_specs=placed,
        out_specs=P(("groups", "res"), "seq", None),
        check_vma=False,
    )
```

```python
import functools
import math

import jax
import jax.numpy as jnp
from jax import lax
from jax.experimental import pallas as pl
from jax.experimental.pallas import tpu as pltpu
from jax.sharding import PartitionSpec as P

F32 = jnp.float32
BF16 = jnp.bfloat16
MESH = pl.DeviceIdType.MESH
LANES = 128
SUBLANES = 8


def kernel(
    n_res, n_seq, x_hbm, gain_hbm, wl_hbm, wr_hbm, w_hbm, bias_hbm, out_ref,
    x_ref, gain_ref, wl_ref, wr_ref, w_ref, bias_ref,
    wide_ref, mixed_ref, left_own, left_got, blocks, right_own, right_got, tall,
    held, early_bytes, late_bytes, load_sem, lrecv_sem, rrecv_sem, ready_sem, *accs,
):
    seqs, res, width = x_ref.shape
    ch = wl_ref.shape[0]
    cz = bias_ref.shape[1]
    pack = LANES // seqs
    high = ch // pack
    half = n_res // n_seq
    rows = res * high
    inv_count = 1.0 / (seqs * n_seq)
    my_res, my_seq = lax.axis_index("res"), lax.axis_index("seq")
    my_col = my_res // half
    first = my_seq * half
    short = n_res <= 8
    levels = ready_sem.shape[0]
    group = math.gcd(half, 4)
    chunks = (len(accs) // 2 - 2) // 2
    step = n_res // levels

    def load(src, dst, n):
        copy = pltpu.make_async_copy(src, dst, load_sem.at[n])
        copy.start()

    def await_bytes(ref, sem):
        pltpu.make_async_copy(ref, ref, sem).wait()

    for n in range(4):
        at = pl.ds(n * (seqs // 4), seqs // 4)
        load(x_hbm.at[at], x_ref.at[at], 0)
    load(wr_hbm, wr_ref, 0)
    load(gain_hbm, gain_ref, 0)
    load(wl_hbm, wl_ref, n_seq)

    barrier = pltpu.get_barrier_semaphore()

    def signal(sem, res_at, seq_at):
        pl.semaphore_signal(
            sem, inc=1, device_id={"res": res_at, "seq": seq_at}, device_id_type=MESH
        )

    for k in range(1, n_seq):
        signal(barrier, my_res, lax.rem(my_seq + k, n_seq))

    def greet(res_at, carry):
        for seq_at in range(n_seq):

            @pl.when((res_at > my_res) & ((my_col == seq_at) | (res_at // half == my_seq)))
            def _():
                signal(barrier, res_at, seq_at)

        return carry

    lax.fori_loop(0, n_res, greet, 0, unroll=short)
    def meet():
        near = jnp.minimum(jnp.maximum(my_res - first, 0), half)
        pl.semaphore_wait(barrier, my_res + (n_seq - 1) * near + n_seq - 1)

        my_level = my_res // step

        def answer(n, carry):
            for seq_at in range(n_seq):

                @pl.when(first + n < my_res)
                def _():
                    signal(ready_sem.at[my_level], first + n, seq_at)

            return carry

        lax.fori_loop(0, half, answer, 0, unroll=short)

    pl.when(my_res % 2 == 1)(meet)

    await_bytes(early_bytes, load_sem.at[0])

    values = x_ref[...].astype(F32).reshape(seqs * res, width)
    side_acc, row_acc, first_acc, second_acc = [
        [accs[q * len(accs) // 2 + n] for q in range(2)] for n in range(2)
    ] + [[accs[q * len(accs) // 2 + 2 + k * chunks : ][:chunks] for q in range(2)] for k in range(2)]
    gained = (wr_ref[...].astype(F32) * gain_ref[...]).astype(BF16)
    sublane = lax.broadcasted_iota(jnp.int32, (SUBLANES, LANES), 0)

    def repeated(j):
        source = sublane // res * res + j
        return jnp.concatenate(
            [
                jnp.concatenate(
                    [
                        jnp.take_along_axis(
                            values[at : at + SUBLANES, n * LANES : (n + 1) * LANES], source, 0
                        )
                        for n in range(width // LANES)
                    ],
                    1,
                )
                for at in range(0, seqs * res, SUBLANES)
            ],
            0,
        ).astype(BF16)

    for q in range(2):
        pltpu.matmul_push_rhs(
            jnp.concatenate([repeated(q * res // 2 + n) for n in range(res // 2)], 0),
            0,
            q,
            transpose=True,
        )
        pltpu.matmul_acc_lhs(side_acc[q], gained, load_staged_rhs=0)
    product = [pltpu.matmul_pop(side_acc[q]) for q in range(2)]
    weight_sum = jnp.sum(gained.astype(F32), axis=-1, keepdims=True)
    mean = jnp.mean(values, axis=-1, keepdims=True)
    centred = values - mean
    variance = jnp.mean(centred * centred, axis=-1, keepdims=True)
    scale = lax.rsqrt(variance + 1e-05)

    lane = lax.broadcasted_iota(jnp.int32, (high, LANES), 1)
    in_group = [lane % pack == g for g in range(pack)]

    def spread(pieces):
        total = pieces[0]
        for g in range(1, pack):
            total = jnp.where(in_group[g], pieces[g], total)
        return total

    per_row = SUBLANES // res
    blocks_at = lax.broadcasted_iota(jnp.int32, (seqs * res // SUBLANES, SUBLANES, LANES), 0)
    row_at = lax.broadcasted_iota(jnp.int32, (seqs * res // SUBLANES, SUBLANES, LANES), 1)
    lane_at = lax.broadcasted_iota(jnp.int32, (seqs * res // SUBLANES, SUBLANES, LANES), 2)
    own = blocks_at * per_row + row_at // res == lane_at // pack

    def to_lanes(column):
        tall = jnp.where(own, column.reshape(seqs * res // SUBLANES, SUBLANES, 1), 0.0)
        tall = jnp.sum(tall, axis=0)
        total = tall[:res]
        for n in range(1, per_row):
            total = total + tall[n * res : (n + 1) * res]
        return total

    sums = spread(
        [
            jnp.broadcast_to(weight_sum[g * high : (g + 1) * high], (high, LANES))
            for g in range(pack)
        ]
    )
    mean_at, scale_at = to_lanes(mean), to_lanes(scale)
    for j in range(res):
        at = j % (res // 2) * LANES
        pieces = [
            product[j * 2 // res][g * high : (g + 1) * high, at : at + LANES] for g in range(pack)
        ]
        total = (spread(pieces) - mean_at[j : j + 1] * sums) * scale_at[j : j + 1]
        tall[pl.ds(j, high, stride=res), :] = total
    right_own[...] = tall[...].astype(BF16)

    my_slot = lax.rem(my_res, half)
    away = lax.rem(my_seq - my_col + n_seq, n_seq)

    def last_slot(res_at):
        return jnp.where(res_at < n_res - half, half - 1, min(1, half - 1))

    def comes_last(res_at):
        return (my_seq == 0) & (my_slot == last_slot(res_at))

    def right_at(res_at):
        return right_got.at[jnp.where(comes_last(res_at), n_res, away * half + my_slot)]

    def right_sem(res_at):
        return rrecv_sem.at[jnp.where(comes_last(res_at), 1, 0)]

    def send_right(res_at):
        return pltpu.make_async_remote_copy(
            src_ref=right_own,
            dst_ref=right_at(res_at),
            send_sem=load_sem.at[0],
            recv_sem=right_sem(res_at),
            device_id={"res": res_at, "seq": my_col},
            device_id_type=MESH,
        )

    def lower(res_at, carry):
        @pl.when(res_at < my_res)
        def _():
            send_right(res_at).start()

        return carry

    pl.when(my_res % 2 == 0)(meet)
    lower(0, 0)
    await_bytes(wl_ref, load_sem.at[n_seq])
    normed = (centred * scale * gain_ref[...]).astype(BF16)
    pltpu.matmul_push_rhs(jnp.concatenate([wl_ref[...]] * (width // ch), 0), 0, 0, transpose=True)
    pltpu.matmul_acc_lhs(row_acc[0], normed, load_staged_rhs=0)
    left_own[...] = pltpu.matmul_pop(row_acc[0])[:, : pack * ch].astype(BF16)
    lax.fori_loop(1, n_res - 1, lower, 0, unroll=short)
    keep = pltpu.make_async_copy(right_own, right_at(my_res), right_sem(my_res))

    @pl.when(away == 0)
    def _():
        keep.start()

    @pl.when(away != 0)
    def _():
        send_right(my_res).start()

    load(w_hbm, w_ref, 1)
    load(bias_hbm, bias_ref, 1)
    last = lax.rem(n_seq - my_seq, n_seq) * half + last_slot(my_res)
    right_got[last] = jnp.zeros((rows, LANES), BF16)
    await_bytes(late_bytes, load_sem.at[1])
    left_sends = []
    for k in range(1, n_seq):
        copy = pltpu.make_async_remote_copy(
            src_ref=left_own,
            dst_ref=left_got.at[n_seq - k - 1],
            send_sem=load_sem.at[k],
            recv_sem=lrecv_sem.at[n_seq - k - 1],
            device_id={"res": my_res, "seq": lax.rem(my_seq + k, n_seq)},
            device_id_type=MESH,
        )
        copy.start()
        left_sends.append(copy)

    wide_ref[...] = w_ref[...].astype(F32)
    for h in range(high):
        for g in range(pack):
            e = g * high + h
            at = (h // per_row * pack + g) * ch
            out_at = h % per_row * cz
            mixed_ref[at : at + ch, out_at : out_at + cz] = wide_ref[
                pl.ds(e, ch, stride=ch), :
            ].astype(BF16)

    for k in range(1, n_seq):
        left_sends[n_seq - k - 1].wait_recv()
    sides = jnp.concatenate([left_own[...]] + [left_got[k - 1] for k in range(1, n_seq)], 0)
    to_row = lax.broadcasted_iota(jnp.int32, (LANES, n_seq * LANES), 0)
    from_row = lax.broadcasted_iota(jnp.int32, (LANES, n_seq * LANES), 1)
    offset = from_row - to_row // pack * res
    copy_at = lax.broadcasted_iota(jnp.int32, (LANES, pack * ch), 1) // ch
    group_at = lax.broadcasted_iota(jnp.int32, (LANES, pack * ch), 0) % pack
    for q in range(2):
        pltpu.matmul_push_rhs(jnp.concatenate([sides] * 2, 1), 0, q)
    for part in range(n_seq):
        for i in range(res):
            q = i % 2
            pick = (offset == part * LANES + i).astype(F32).astype(BF16)
            pltpu.matmul_acc_lhs(
                row_acc[q], pick, load_staged_rhs=0 if part == 0 and i < 2 else None
            )
            block = pltpu.matmul_pop(row_acc[q])[:, : pack * ch]
            blocks[part * LANES : (part + 1) * LANES, i * pack * ch : (i + 1) * pack * ch] = (
                jnp.where(group_at == copy_at, block, 0.0).astype(BF16)
            )

    for level in range(levels):
        above = jnp.minimum((level + 1) * step - 1 - my_res, step)

        @pl.when(above > 0)
        def _():
            pl.semaphore_wait(ready_sem.at[level], above)

            def higher(n, carry):
                @pl.when(level * step + n > my_res)
                def _():
                    send_right(level * step + n).start()

                return carry

            lax.fori_loop(0, step, higher, 0, unroll=short)

    tiles = high // per_row
    wide = 2 * LANES

    def push_weights():
        for q in range(2):
            pltpu.matmul_push_rhs(blocks[:, q * wide : (q + 1) * wide], 0, q)
            pltpu.matmul_push_rhs(mixed_ref[q * wide : (q + 1) * wide, :], 1, q)

    def first_matmul(n, lhs):
        for q in range(2):
            pltpu.matmul_acc_lhs(first_acc[q][n], lhs, load_staged_rhs=None if n else 0)

    def second_matmul(n, lhs):
        for q in range(2):
            pltpu.matmul_acc_lhs(second_acc[q][n], lhs[q], load_staged_rhs=None if n else 1)

    def second_result(n):
        both = pltpu.matmul_pop(second_acc[0][n]) + pltpu.matmul_pop(second_acc[1][n])
        found = []
        for at in range(0, 2 * SUBLANES, SUBLANES):
            piece = both[at : at + res, :cz]
            for h in range(1, per_row):
                piece = piece + both[at + h * res : at + (h + 1) * res, h * cz : (h + 1) * cz]
            found.append(piece)
        return found

    def lanes_of(outer, i):
        return outer[i // 2][:, i % 2 * LANES : (i % 2 + 1) * LANES]

    def columns(n):
        pairs = range(group // 2)
        for pair in pairs:
            for tile in range(tiles):
                lhs = [
                    right_got[
                        pl.ds(part * half + n * group + 2 * pair, 2),
                        tile * SUBLANES : (tile + 1) * SUBLANES,
                    ].reshape(2 * SUBLANES, LANES)
                    for part in range(n_seq)
                ]
                first_matmul(pair * tiles + tile, jnp.concatenate(lhs, 1))
        outer = [
            [pltpu.matmul_pop(first_acc[q][k]) for q in range(2)] for k in range(len(pairs) * tiles)
        ]
        for pair in pairs:
            for i in range(res):
                lhs = [
                    jnp.concatenate(
                        [
                            lanes_of(outer[pair * tiles + 2 * q + tile], i).astype(BF16)
                            for tile in range(tiles // 2)
                        ],
                        1,
                    )
                    for q in range(2)
                ]
                second_matmul(pair * res + i, lhs)
        for pair in pairs:
            for i in range(res):
                found = second_result(pair * res + i)
                at = pl.ds(pl.multiple_of((n * group + 2 * pair) * res, SUBLANES), SUBLANES)
                held[i, at, :] = jnp.concatenate(found, 0) * inv_count + bias_ref[...]

    if half == group:
        push_weights()
        await_bytes(right_got.at[pl.ds(0, n_res - 1)], rrecv_sem.at[0])
        columns(0)
    else:
        await_bytes(right_got.at[pl.ds(0, n_res - 1)], rrecv_sem.at[0])

        @pl.loop(0, half // group)
        def _(n):
            push_weights()
            columns(n)

    push_weights()
    my_last = last_slot(my_res)
    my_part = lax.rem(n_seq - my_seq, n_seq)
    await_bytes(right_got.at[n_res], rrecv_sem.at[1])
    for pair in range(tiles // 2):
        block = right_got[n_res, pair * 2 * SUBLANES : (pair + 1) * 2 * SUBLANES, :]
        zero = jnp.zeros_like(block)
        lhs = [jnp.where(my_part == part, block, zero) for part in range(n_seq)]
        first_matmul(pair, jnp.concatenate(lhs, 1))
    outer = [[pltpu.matmul_pop(first_acc[q][k]) for q in range(2)] for k in range(tiles // 2)]
    for pair in range(res // 2):
        lhs = []
        for q in range(2):
            pieces = []
            for tile in range(tiles // 2):
                at = slice(tile * SUBLANES, (tile + 1) * SUBLANES)
                pieces.append(
                    jnp.concatenate(
                        [lanes_of(outer[q], 2 * pair + k)[at] for k in range(2)], 0
                    ).astype(BF16)
                )
            lhs.append(jnp.concatenate(pieces, 1))
        second_matmul(pair, lhs)
    found = [piece for pair in range(res // 2) for piece in second_result(pair)]

    def finish(n):
        for i in range(res):
            piece = found[i] * inv_count
            for pair in range(group // 2):
                slot = n * group + 2 * pair
                at = pl.ds(pl.multiple_of(slot * res, SUBLANES), SUBLANES)
                added = [jnp.where(my_last == slot + k, piece, 0.0) for k in range(2)]
                out_ref[i, at, :] = (held[i, at, :] + jnp.concatenate(added, 0)).astype(BF16)

    if half == group:
        finish(0)
    else:

        @pl.loop(0, half // group)
        def _(n):
            finish(n)

    for copy in left_sends:
        copy.wait_send()

    @pl.when(away == 0)
    def _():
        await_bytes(right_got.at[pl.ds(0, n_res - 1)], load_sem.at[0])

    @pl.when(away != 0)
    def _():
        await_bytes(right_got.at[pl.ds(0, n_res)], load_sem.at[0])


def scoped(n_res, n_seq, *refs):
    accumulators = [
        pltpu.ACC(q)((m, 2 * LANES), F32) for q in range(2) for m in [32, LANES] + [16] * 16
    ]
    pl.run_scoped(
        functools.partial(kernel, n_res, n_seq, *refs),
        pltpu.SemaphoreType.DMA((n_seq + 1,)),
        pltpu.SemaphoreType.DMA((n_seq - 1,)),
        pltpu.SemaphoreType.DMA((2,)),
        pltpu.SemaphoreType.REGULAR((2 * n_seq,)),
        *accumulators,
    )


def on_device(alignment, ln_gain, proj_left, proj_right, out_weight, out_bias):
    n_res, n_seq = lax.axis_size("res"), lax.axis_size("seq")
    seqs, res, width = alignment.shape
    ch = proj_left.shape[1]
    cz = out_weight.shape[1]
    half = n_res // n_seq
    cols = res * half
    pack = LANES // seqs
    rows = res * (ch // pack)
    wide = res * pack * ch
    group = math.gcd(half, 4)
    per_row = SUBLANES // res
    unit = 2 * LANES * 4
    early = (seqs * res * width + ch * width) * 2 + width * 4
    late = ch * ch * cz * 2 + cz * 4
    return pl.pallas_call(
        functools.partial(scoped, n_res, n_seq),
        out_shape=pltpu.VMEM((res, cols, cz), BF16),
        in_specs=[pl.BlockSpec(memory_space=pl.ANY)] * 6,
        out_specs=pl.BlockSpec(memory_space=pltpu.VMEM),
        scratch_shapes=[
            pltpu.VMEM((seqs, res, width), BF16),
            pltpu.VMEM((1, width), F32),
            pltpu.VMEM((ch, width), BF16),
            pltpu.VMEM((ch, width), BF16),
            pltpu.VMEM((ch * ch, cz), BF16),
            pltpu.VMEM((1, cz), F32),
            pltpu.VMEM((ch * ch, cz), F32),
            pltpu.VMEM((ch * ch // per_row, per_row * cz), BF16),
            pltpu.VMEM((res * seqs, pack * ch), BF16),
            pltpu.VMEM((n_seq - 1, res * seqs, pack * ch), BF16),
            pltpu.VMEM((n_seq * LANES, wide), BF16),
            pltpu.VMEM((rows, LANES), BF16),
            pltpu.VMEM((n_res + 1, rows, LANES), BF16),
            pltpu.VMEM((rows, LANES), F32),
            pltpu.VMEM((res, cols, cz), F32),
            pltpu.VMEM((early // unit, 2, LANES), F32),
            pltpu.VMEM((late // (unit // 2), 1, LANES), F32),
        ],
        compiler_params=pltpu.CompilerParams(collective_id=0, has_side_effects=True),
    )(
        alignment,
        ln_gain.reshape(1, width),
        proj_left.T,
        proj_right.T,
        out_weight,
        out_bias.reshape(1, cz),
    )


def solution(mesh):
    placed = (P(("groups", "seq"), "res", None), P(), P(), P(), P(), P())
    return jax.shard_map(
        on_device,
        mesh=mesh,
        in_specs=placed,
        out_specs=P(("groups", "res"), "seq", None),
        check_vma=False,
    )
```

```python
import functools
import math

import jax
import jax.numpy as jnp
from jax import lax
from jax.experimental import pallas as pl
from jax.experimental.pallas import tpu as pltpu
from jax.sharding import PartitionSpec as P

F32 = jnp.float32
BF16 = jnp.bfloat16
MESH = pl.DeviceIdType.MESH
LANES = 128
SUBLANES = 8


def kernel(
    n_res, n_seq, x_hbm, gain_hbm, wl_hbm, wr_hbm, w_hbm, bias_hbm, out_ref,
    x_ref, gain_ref, wl_ref, wr_ref, w_ref, bias_ref,
    wide_ref, mixed_ref, left_own, left_got, blocks, right_own, right_got, tall,
    held, early_bytes, late_bytes, load_sem, lrecv_sem, rrecv_sem, ready_sem, *accs,
):
    seqs, res, width = x_ref.shape
    ch = wl_ref.shape[0]
    cz = bias_ref.shape[1]
    pack = LANES // seqs
    high = ch // pack
    half = n_res // n_seq
    rows = res * high
    inv_count = 1.0 / (seqs * n_seq)
    my_res, my_seq = lax.axis_index("res"), lax.axis_index("seq")
    my_col = my_res // half
    first = my_seq * half
    short = n_res <= 8
    levels = ready_sem.shape[0]
    group = math.gcd(half, 4)
    chunks = (len(accs) // 2 - 2) // 2
    step = n_res // levels

    def load(src, dst, n):
        copy = pltpu.make_async_copy(src, dst, load_sem.at[n])
        copy.start()

    def await_bytes(ref, sem):
        pltpu.make_async_copy(ref, ref, sem).wait()

    for n in range(2):
        at = pl.ds(n * (seqs // 2), seqs // 2)
        load(x_hbm.at[at], x_ref.at[at], 0)
    for n in range(2):
        at = pl.ds(n * (ch // 2), ch // 2)
        load(wr_hbm.at[at], wr_ref.at[at], 0)
    load(gain_hbm, gain_ref, 0)
    load(wl_hbm, wl_ref, n_seq)

    barrier = pltpu.get_barrier_semaphore()

    def signal(sem, res_at, seq_at):
        pl.semaphore_signal(
            sem, inc=1, device_id={"res": res_at, "seq": seq_at}, device_id_type=MESH
        )

    for k in range(1, n_seq):
        signal(barrier, my_res, lax.rem(my_seq + k, n_seq))

    def greet(res_at, carry):
        for seq_at in range(n_seq):

            @pl.when((res_at > my_res) & ((my_col == seq_at) | (res_at // half == my_seq)))
            def _():
                signal(barrier, res_at, seq_at)

        return carry

    lax.fori_loop(0, n_res, greet, 0, unroll=short)
    def meet():
        near = jnp.minimum(jnp.maximum(my_res - first, 0), half)
        pl.semaphore_wait(barrier, my_res + (n_seq - 1) * near + n_seq - 1)

        my_level = my_res // step

        def answer(n, carry):
            for seq_at in range(n_seq):

                @pl.when(first + n < my_res)
                def _():
                    signal(ready_sem.at[my_level], first + n, seq_at)

            return carry

        lax.fori_loop(0, half, answer, 0, unroll=short)

    pl.when(my_res % 2 == 1)(meet)

    await_bytes(early_bytes, load_sem.at[0])

    values = x_ref[...].astype(F32).reshape(seqs * res, width)
    side_acc, row_acc, first_acc, second_acc = [
        [accs[q * len(accs) // 2 + n] for q in range(2)] for n in range(2)
    ] + [[accs[q * len(accs) // 2 + 2 + k * chunks : ][:chunks] for q in range(2)] for k in range(2)]
    gained = (wr_ref[...].astype(F32) * gain_ref[...]).astype(BF16)
    sublane = lax.broadcasted_iota(jnp.int32, (SUBLANES, LANES), 0)

    def repeated(j):
        source = sublane // res * res + j
        return jnp.concatenate(
            [
                jnp.concatenate(
                    [
                        jnp.take_along_axis(
                            values[at : at + SUBLANES, n * LANES : (n + 1) * LANES], source, 0
                        )
                        for n in range(width // LANES)
                    ],
                    1,
                )
                for at in range(0, seqs * res, SUBLANES)
            ],
            0,
        ).astype(BF16)

    for q in range(2):
        pltpu.matmul_push_rhs(
            jnp.concatenate([repeated(q * res // 2 + n) for n in range(res // 2)], 0),
            0,
            q,
            transpose=True,
        )
        pltpu.matmul_acc_lhs(side_acc[q], gained, load_staged_rhs=0)
    product = [pltpu.matmul_pop(side_acc[q]) for q in range(2)]
    weight_sum = jnp.sum(gained.astype(F32), axis=-1, keepdims=True)
    mean = jnp.mean(values, axis=-1, keepdims=True)
    centred = values - mean
    variance = jnp.mean(centred * centred, axis=-1, keepdims=True)
    scale = lax.rsqrt(variance + 1e-05)

    lane = lax.broadcasted_iota(jnp.int32, (high, LANES), 1)
    in_group = [lane % pack == g for g in range(pack)]

    def spread(pieces):
        total = pieces[0]
        for g in range(1, pack):
            total = jnp.where(in_group[g], pieces[g], total)
        return total

    per_row = SUBLANES // res
    blocks_at = lax.broadcasted_iota(jnp.int32, (seqs * res // SUBLANES, SUBLANES, LANES), 0)
    row_at = lax.broadcasted_iota(jnp.int32, (seqs * res // SUBLANES, SUBLANES, LANES), 1)
    lane_at = lax.broadcasted_iota(jnp.int32, (seqs * res // SUBLANES, SUBLANES, LANES), 2)
    own = blocks_at * per_row + row_at // res == lane_at // pack

    def to_lanes(column):
        tall = jnp.where(own, column.reshape(seqs * res // SUBLANES, SUBLANES, 1), 0.0)
        tall = jnp.sum(tall, axis=0)
        total = tall[:res]
        for n in range(1, per_row):
            total = total + tall[n * res : (n + 1) * res]
        return total

    sums = spread(
        [
            jnp.broadcast_to(weight_sum[g * high : (g + 1) * high], (high, LANES))
            for g in range(pack)
        ]
    )
    mean_at, scale_at = to_lanes(mean), to_lanes(scale)
    for j in range(res):
        at = j % (res // 2) * LANES
        pieces = [
            product[j * 2 // res][g * high : (g + 1) * high, at : at + LANES] for g in range(pack)
        ]
        total = (spread(pieces) - mean_at[j : j + 1] * sums) * scale_at[j : j + 1]
        tall[pl.ds(j, high, stride=res), :] = total
    right_own[...] = tall[...].astype(BF16)

    my_slot = lax.rem(my_res, half)
    away = lax.rem(my_seq - my_col + n_seq, n_seq)

    def last_slot(res_at):
        return jnp.where(res_at < n_res - half, half - 1, min(1, half - 1))

    def comes_last(res_at):
        return (my_seq == 0) & (my_slot == last_slot(res_at))

    def right_at(res_at):
        return right_got.at[jnp.where(comes_last(res_at), n_res, away * half + my_slot)]

    def right_sem(res_at):
        return rrecv_sem.at[jnp.where(comes_last(res_at), 1, 0)]

    def send_right(res_at):
        return pltpu.make_async_remote_copy(
            src_ref=right_own,
            dst_ref=right_at(res_at),
            send_sem=load_sem.at[0],
            recv_sem=right_sem(res_at),
            device_id={"res": res_at, "seq": my_col},
            device_id_type=MESH,
        )

    def lower(res_at, carry):
        @pl.when(res_at < my_res)
        def _():
            send_right(res_at).start()

        return carry

    pl.when(my_res % 2 == 0)(meet)
    lower(0, 0)
    await_bytes(wl_ref, load_sem.at[n_seq])
    normed = (centred * scale * gain_ref[...]).astype(BF16)
    pltpu.matmul_push_rhs(jnp.concatenate([wl_ref[...]] * (width // ch), 0), 0, 0, transpose=True)
    pltpu.matmul_acc_lhs(row_acc[0], normed, load_staged_rhs=0)
    left_own[...] = pltpu.matmul_pop(row_acc[0])[:, : pack * ch].astype(BF16)
    lax.fori_loop(1, n_res - 1, lower, 0, unroll=short)
    keep = pltpu.make_async_copy(right_own, right_at(my_res), right_sem(my_res))

    @pl.when(away == 0)
    def _():
        keep.start()

    @pl.when(away != 0)
    def _():
        send_right(my_res).start()

    load(w_hbm, w_ref, 1)
    load(bias_hbm, bias_ref, 1)
    last = lax.rem(n_seq - my_seq, n_seq) * half + last_slot(my_res)
    right_got[last] = jnp.zeros((rows, LANES), BF16)
    await_bytes(late_bytes, load_sem.at[1])
    left_sends = []
    for k in range(1, n_seq):
        copy = pltpu.make_async_remote_copy(
            src_ref=left_own,
            dst_ref=left_got.at[n_seq - k - 1],
            send_sem=load_sem.at[k],
            recv_sem=lrecv_sem.at[n_seq - k - 1],
            device_id={"res": my_res, "seq": lax.rem(my_seq + k, n_seq)},
            device_id_type=MESH,
        )
        copy.start()
        left_sends.append(copy)

    wide_ref[...] = w_ref[...].astype(F32)
    for h in range(high):
        for g in range(pack):
            e = g * high + h
            at = (h // per_row * pack + g) * ch
            out_at = h % per_row * cz
            mixed_ref[at : at + ch, out_at : out_at + cz] = wide_ref[
                pl.ds(e, ch, stride=ch), :
            ].astype(BF16)

    for k in range(1, n_seq):
        left_sends[n_seq - k - 1].wait_recv()
    sides = jnp.concatenate([left_own[...]] + [left_got[k - 1] for k in range(1, n_seq)], 0)
    to_row = lax.broadcasted_iota(jnp.int32, (LANES, n_seq * LANES), 0)
    from_row = lax.broadcasted_iota(jnp.int32, (LANES, n_seq * LANES), 1)
    offset = from_row - to_row // pack * res
    copy_at = lax.broadcasted_iota(jnp.int32, (LANES, pack * ch), 1) // ch
    group_at = lax.broadcasted_iota(jnp.int32, (LANES, pack * ch), 0) % pack
    for q in range(2):
        pltpu.matmul_push_rhs(jnp.concatenate([sides] * 2, 1), 0, q)
    for part in range(n_seq):
        for i in range(res):
            q = i % 2
            pick = (offset == part * LANES + i).astype(F32).astype(BF16)
            pltpu.matmul_acc_lhs(
                row_acc[q], pick, load_staged_rhs=0 if part == 0 and i < 2 else None
            )
            block = pltpu.matmul_pop(row_acc[q])[:, : pack * ch]
            blocks[part * LANES : (part + 1) * LANES, i * pack * ch : (i + 1) * pack * ch] = (
                jnp.where(group_at == copy_at, block, 0.0).astype(BF16)
            )

    for level in range(levels):
        above = jnp.minimum((level + 1) * step - 1 - my_res, step)

        @pl.when(above > 0)
        def _():
            pl.semaphore_wait(ready_sem.at[level], above)

            def higher(n, carry):
                @pl.when(level * step + n > my_res)
                def _():
                    send_right(level * step + n).start()

                return carry

            lax.fori_loop(0, step, higher, 0, unroll=short)

    tiles = high // per_row
    wide = 2 * LANES

    def push_weights():
        for q in range(2):
            pltpu.matmul_push_rhs(blocks[:, q * wide : (q + 1) * wide], 0, q)
            pltpu.matmul_push_rhs(mixed_ref[q * wide : (q + 1) * wide, :], 1, q)

    def first_matmul(n, lhs):
        for q in range(2):
            pltpu.matmul_acc_lhs(first_acc[q][n], lhs, load_staged_rhs=None if n else 0)

    def second_matmul(n, lhs):
        for q in range(2):
            pltpu.matmul_acc_lhs(second_acc[q][n], lhs[q], load_staged_rhs=None if n else 1)

    def second_result(n):
        both = pltpu.matmul_pop(second_acc[0][n]) + pltpu.matmul_pop(second_acc[1][n])
        found = []
        for at in range(0, 2 * SUBLANES, SUBLANES):
            piece = both[at : at + res, :cz]
            for h in range(1, per_row):
                piece = piece + both[at + h * res : at + (h + 1) * res, h * cz : (h + 1) * cz]
            found.append(piece)
        return found

    def lanes_of(outer, i):
        return outer[i // 2][:, i % 2 * LANES : (i % 2 + 1) * LANES]

    def columns(n):
        pairs = range(group // 2)
        for pair in pairs:
            for tile in range(tiles):
                lhs = [
                    right_got[
                        pl.ds(part * half + n * group + 2 * pair, 2),
                        tile * SUBLANES : (tile + 1) * SUBLANES,
                    ].reshape(2 * SUBLANES, LANES)
                    for part in range(n_seq)
                ]
                first_matmul(pair * tiles + tile, jnp.concatenate(lhs, 1))
        outer = [
            [pltpu.matmul_pop(first_acc[q][k]) for q in range(2)] for k in range(len(pairs) * tiles)
        ]
        for pair in pairs:
            for i in range(res):
                lhs = [
                    jnp.concatenate(
                        [
                            lanes_of(outer[pair * tiles + 2 * q + tile], i).astype(BF16)
                            for tile in range(tiles // 2)
                        ],
                        1,
                    )
                    for q in range(2)
                ]
                second_matmul(pair * res + i, lhs)
        for pair in pairs:
            for i in range(res):
                found = second_result(pair * res + i)
                at = pl.ds(pl.multiple_of((n * group + 2 * pair) * res, SUBLANES), SUBLANES)
                held[i, at, :] = jnp.concatenate(found, 0) * inv_count + bias_ref[...]

    if half == group:
        push_weights()
        await_bytes(right_got.at[pl.ds(0, n_res - 1)], rrecv_sem.at[0])
        columns(0)
    else:
        await_bytes(right_got.at[pl.ds(0, n_res - 1)], rrecv_sem.at[0])

        @pl.loop(0, half // group)
        def _(n):
            push_weights()
            columns(n)

    push_weights()
    my_last = last_slot(my_res)
    my_part = lax.rem(n_seq - my_seq, n_seq)
    await_bytes(right_got.at[n_res], rrecv_sem.at[1])
    for pair in range(tiles // 2):
        block = right_got[n_res, pair * 2 * SUBLANES : (pair + 1) * 2 * SUBLANES, :]
        zero = jnp.zeros_like(block)
        lhs = [jnp.where(my_part == part, block, zero) for part in range(n_seq)]
        first_matmul(pair, jnp.concatenate(lhs, 1))
    outer = [[pltpu.matmul_pop(first_acc[q][k]) for q in range(2)] for k in range(tiles // 2)]
    for pair in range(res // 2):
        lhs = []
        for q in range(2):
            pieces = []
            for tile in range(tiles // 2):
                at = slice(tile * SUBLANES, (tile + 1) * SUBLANES)
                pieces.append(
                    jnp.concatenate(
                        [lanes_of(outer[q], 2 * pair + k)[at] for k in range(2)], 0
                    ).astype(BF16)
                )
            lhs.append(jnp.concatenate(pieces, 1))
        second_matmul(pair, lhs)
    found = [piece for pair in range(res // 2) for piece in second_result(pair)]

    def finish(n):
        for i in range(res):
            piece = found[i] * inv_count
            for pair in range(group // 2):
                slot = n * group + 2 * pair
                at = pl.ds(pl.multiple_of(slot * res, SUBLANES), SUBLANES)
                added = [jnp.where(my_last == slot + k, piece, 0.0) for k in range(2)]
                out_ref[i, at, :] = (held[i, at, :] + jnp.concatenate(added, 0)).astype(BF16)

    if half == group:
        finish(0)
    else:

        @pl.loop(0, half // group)
        def _(n):
            finish(n)

    for copy in left_sends:
        copy.wait_send()

    @pl.when(away == 0)
    def _():
        await_bytes(right_got.at[pl.ds(0, n_res - 1)], load_sem.at[0])

    @pl.when(away != 0)
    def _():
        await_bytes(right_got.at[pl.ds(0, n_res)], load_sem.at[0])


def scoped(n_res, n_seq, *refs):
    accumulators = [
        pltpu.ACC(q)((m, 2 * LANES), F32) for q in range(2) for m in [32, LANES] + [16] * 16
    ]
    pl.run_scoped(
        functools.partial(kernel, n_res, n_seq, *refs),
        pltpu.SemaphoreType.DMA((n_seq + 1,)),
        pltpu.SemaphoreType.DMA((n_seq - 1,)),
        pltpu.SemaphoreType.DMA((2,)),
        pltpu.SemaphoreType.REGULAR((2 * n_seq,)),
        *accumulators,
    )


def on_device(alignment, ln_gain, proj_left, proj_right, out_weight, out_bias):
    n_res, n_seq = lax.axis_size("res"), lax.axis_size("seq")
    seqs, res, width = alignment.shape
    ch = proj_left.shape[1]
    cz = out_weight.shape[1]
    half = n_res // n_seq
    cols = res * half
    pack = LANES // seqs
    rows = res * (ch // pack)
    wide = res * pack * ch
    group = math.gcd(half, 4)
    per_row = SUBLANES // res
    unit = 2 * LANES * 4
    early = (seqs * res * width + ch * width) * 2 + width * 4
    late = ch * ch * cz * 2 + cz * 4
    return pl.pallas_call(
        functools.partial(scoped, n_res, n_seq),
        out_shape=pltpu.VMEM((res, cols, cz), BF16),
        in_specs=[pl.BlockSpec(memory_space=pl.ANY)] * 6,
        out_specs=pl.BlockSpec(memory_space=pltpu.VMEM),
        scratch_shapes=[
            pltpu.VMEM((seqs, res, width), BF16),
            pltpu.VMEM((1, width), F32),
            pltpu.VMEM((ch, width), BF16),
            pltpu.VMEM((ch, width), BF16),
            pltpu.VMEM((ch * ch, cz), BF16),
            pltpu.VMEM((1, cz), F32),
            pltpu.VMEM((ch * ch, cz), F32),
            pltpu.VMEM((ch * ch // per_row, per_row * cz), BF16),
            pltpu.VMEM((res * seqs, pack * ch), BF16),
            pltpu.VMEM((n_seq - 1, res * seqs, pack * ch), BF16),
            pltpu.VMEM((n_seq * LANES, wide), BF16),
            pltpu.VMEM((rows, LANES), BF16),
            pltpu.VMEM((n_res + 1, rows, LANES), BF16),
            pltpu.VMEM((rows, LANES), F32),
            pltpu.VMEM((res, cols, cz), F32),
            pltpu.VMEM((early // unit, 2, LANES), F32),
            pltpu.VMEM((late // (unit // 2), 1, LANES), F32),
        ],
        compiler_params=pltpu.CompilerParams(collective_id=0, has_side_effects=True),
    )(
        alignment,
        ln_gain.reshape(1, width),
        proj_left.T,
        proj_right.T,
        out_weight,
        out_bias.reshape(1, cz),
    )


def solution(mesh):
    placed = (P(("groups", "seq"), "res", None), P(), P(), P(), P(), P())
    return jax.shard_map(
        on_device,
        mesh=mesh,
        in_specs=placed,
        out_specs=P(("groups", "res"), "seq", None),
        check_vma=False,
    )
```

```python
import functools
import math

import jax
import jax.numpy as jnp
from jax import lax
from jax.experimental import pallas as pl
from jax.experimental.pallas import tpu as pltpu
from jax.sharding import PartitionSpec as P

F32 = jnp.float32
BF16 = jnp.bfloat16
MESH = pl.DeviceIdType.MESH
LANES = 128
SUBLANES = 8


def kernel(
    n_res, n_seq, x_hbm, gain_hbm, wl_hbm, wr_hbm, w_hbm, bias_hbm, out_ref,
    x_ref, gain_ref, wl_ref, wr_ref, w_ref, bias_ref,
    wide_ref, mixed_ref, left_own, left_got, blocks, right_own, right_got, tall,
    held, early_bytes, late_bytes, load_sem, lrecv_sem, rrecv_sem, ready_sem, *accs,
):
    seqs, res, width = x_ref.shape
    ch = wl_ref.shape[0]
    cz = bias_ref.shape[1]
    pack = LANES // seqs
    high = ch // pack
    half = n_res // n_seq
    rows = res * high
    inv_count = 1.0 / (seqs * n_seq)
    my_res, my_seq = lax.axis_index("res"), lax.axis_index("seq")
    my_col = my_res // half
    first = my_seq * half
    short = n_res <= 8
    levels = ready_sem.shape[0]
    group = math.gcd(half, 4)
    chunks = (len(accs) // 2 - 2) // 2
    step = n_res // levels

    def load(src, dst, n):
        copy = pltpu.make_async_copy(src, dst, load_sem.at[n])
        copy.start()

    def await_bytes(ref, sem):
        pltpu.make_async_copy(ref, ref, sem).wait()

    for n in range(2):
        at = pl.ds(n * (seqs // 2), seqs // 2)
        load(x_hbm.at[at], x_ref.at[at], 0)
    load(wr_hbm, wr_ref, 0)
    load(gain_hbm, gain_ref, 0)
    load(wl_hbm, wl_ref, n_seq)

    barrier = pltpu.get_barrier_semaphore()

    def signal(sem, res_at, seq_at):
        pl.semaphore_signal(
            sem, inc=1, device_id={"res": res_at, "seq": seq_at}, device_id_type=MESH
        )

    for k in range(1, n_seq):
        signal(barrier, my_res, lax.rem(my_seq + k, n_seq))

    def greet(res_at, carry):
        for seq_at in range(n_seq):

            @pl.when((res_at > my_res) & ((my_col == seq_at) | (res_at // half == my_seq)))
            def _():
                signal(barrier, res_at, seq_at)

        return carry

    lax.fori_loop(0, n_res, greet, 0, unroll=short)
    def meet():
        near = jnp.minimum(jnp.maximum(my_res - first, 0), half)
        pl.semaphore_wait(barrier, my_res + (n_seq - 1) * near + n_seq - 1)

        my_level = my_res // step

        def answer(n, carry):
            for seq_at in range(n_seq):

                @pl.when(first + n < my_res)
                def _():
                    signal(ready_sem.at[my_level], first + n, seq_at)

            return carry

        lax.fori_loop(0, half, answer, 0, unroll=short)

    pl.when(my_res % 2 == 1)(meet)

    await_bytes(early_bytes, load_sem.at[0])

    values = x_ref[...].astype(F32).reshape(seqs * res, width)
    side_acc, row_acc, first_acc, second_acc = [
        [accs[q * len(accs) // 2 + n] for q in range(2)] for n in range(2)
    ] + [[accs[q * len(accs) // 2 + 2 + k * chunks : ][:chunks] for q in range(2)] for k in range(2)]
    gained = (wr_ref[...].astype(F32) * gain_ref[...]).astype(BF16)
    sublane = lax.broadcasted_iota(jnp.int32, (SUBLANES, LANES), 0)

    def repeated(j):
        source = sublane // res * res + j
        return jnp.concatenate(
            [
                jnp.concatenate(
                    [
                        jnp.take_along_axis(
                            values[at : at + SUBLANES, n * LANES : (n + 1) * LANES], source, 0
                        )
                        for n in range(width // LANES)
                    ],
                    1,
                )
                for at in range(0, seqs * res, SUBLANES)
            ],
            0,
        ).astype(BF16)

    for q in range(2):
        pltpu.matmul_push_rhs(
            jnp.concatenate([repeated(q * res // 2 + n) for n in range(res // 2)], 0),
            0,
            q,
            transpose=True,
        )
        pltpu.matmul_acc_lhs(side_acc[q], gained, load_staged_rhs=0)
    product = [pltpu.matmul_pop(side_acc[q]) for q in range(2)]
    weight_sum = jnp.sum(gained.astype(F32), axis=-1, keepdims=True)
    mean = jnp.mean(values, axis=-1, keepdims=True)
    centred = values - mean
    variance = jnp.mean(centred * centred, axis=-1, keepdims=True)
    scale = lax.rsqrt(variance + 1e-05)

    lane = lax.broadcasted_iota(jnp.int32, (high, LANES), 1)
    in_group = [lane % pack == g for g in range(pack)]

    def spread(pieces):
        total = pieces[0]
        for g in range(1, pack):
            total = jnp.where(in_group[g], pieces[g], total)
        return total

    per_row = SUBLANES // res
    blocks_at = lax.broadcasted_iota(jnp.int32, (seqs * res // SUBLANES, SUBLANES, LANES), 0)
    row_at = lax.broadcasted_iota(jnp.int32, (seqs * res // SUBLANES, SUBLANES, LANES), 1)
    lane_at = lax.broadcasted_iota(jnp.int32, (seqs * res // SUBLANES, SUBLANES, LANES), 2)
    own = blocks_at * per_row + row_at // res == lane_at // pack

    def to_lanes(column):
        tall = jnp.where(own, column.reshape(seqs * res // SUBLANES, SUBLANES, 1), 0.0)
        tall = jnp.sum(tall, axis=0)
        total = tall[:res]
        for n in range(1, per_row):
            total = total + tall[n * res : (n + 1) * res]
        return total

    sums = spread(
        [
            jnp.broadcast_to(weight_sum[g * high : (g + 1) * high], (high, LANES))
            for g in range(pack)
        ]
    )
    mean_at, scale_at = to_lanes(mean), to_lanes(scale)
    for j in range(res):
        at = j % (res // 2) * LANES
        pieces = [
            product[j * 2 // res][g * high : (g + 1) * high, at : at + LANES] for g in range(pack)
        ]
        total = (spread(pieces) - mean_at[j : j + 1] * sums) * scale_at[j : j + 1]
        tall[pl.ds(j, high, stride=res), :] = total
    right_own[...] = tall[...].astype(BF16)

    my_slot = lax.rem(my_res, half)
    away = lax.rem(my_seq - my_col + n_seq, n_seq)

    def last_slot(res_at):
        return jnp.where(res_at < n_res - half, half - 1, min(1, half - 1))

    def comes_last(res_at):
        return (my_seq == 0) & (my_slot == last_slot(res_at))

    def right_at(res_at):
        return right_got.at[jnp.where(comes_last(res_at), n_res, away * half + my_slot)]

    def right_sem(res_at):
        return rrecv_sem.at[jnp.where(comes_last(res_at), 1, 0)]

    def send_right(res_at):
        return pltpu.make_async_remote_copy(
            src_ref=right_own,
            dst_ref=right_at(res_at),
            send_sem=load_sem.at[0],
            recv_sem=right_sem(res_at),
            device_id={"res": res_at, "seq": my_col},
            device_id_type=MESH,
        )

    def lower(res_at, carry):
        @pl.when(res_at < my_res)
        def _():
            send_right(res_at).start()

        return carry

    pl.when(my_res % 2 == 0)(meet)
    lower(0, 0)
    await_bytes(wl_ref, load_sem.at[n_seq])
    normed = (centred * scale * gain_ref[...]).astype(BF16)
    pltpu.matmul_push_rhs(jnp.concatenate([wl_ref[...]] * (width // ch), 0), 0, 0, transpose=True)
    pltpu.matmul_acc_lhs(row_acc[0], normed, load_staged_rhs=0)
    left_own[...] = pltpu.matmul_pop(row_acc[0])[:, : pack * ch].astype(BF16)
    lax.fori_loop(1, n_res - 1, lower, 0, unroll=short)
    keep = pltpu.make_async_copy(right_own, right_at(my_res), right_sem(my_res))

    @pl.when(away == 0)
    def _():
        keep.start()

    @pl.when(away != 0)
    def _():
        send_right(my_res).start()

    load(w_hbm, w_ref, 1)
    load(bias_hbm, bias_ref, 1)
    last = lax.rem(n_seq - my_seq, n_seq) * half + last_slot(my_res)
    right_got[last] = jnp.zeros((rows, LANES), BF16)
    await_bytes(late_bytes, load_sem.at[1])
    left_sends = []
    for k in range(1, n_seq):
        copy = pltpu.make_async_remote_copy(
            src_ref=left_own,
            dst_ref=left_got.at[n_seq - k - 1],
            send_sem=load_sem.at[k],
            recv_sem=lrecv_sem.at[n_seq - k - 1],
            device_id={"res": my_res, "seq": lax.rem(my_seq + k, n_seq)},
            device_id_type=MESH,
        )
        copy.start()
        left_sends.append(copy)

    wide_ref[...] = w_ref[...].astype(F32)
    for h in range(high):
        for g in range(pack):
            e = g * high + h
            at = (h // per_row * pack + g) * ch
            out_at = h % per_row * cz
            mixed_ref[at : at + ch, out_at : out_at + cz] = wide_ref[
                pl.ds(e, ch, stride=ch), :
            ].astype(BF16)

    for k in range(1, n_seq):
        left_sends[n_seq - k - 1].wait_recv()
    sides = jnp.concatenate([left_own[...]] + [left_got[k - 1] for k in range(1, n_seq)], 0)
    to_row = lax.broadcasted_iota(jnp.int32, (LANES, n_seq * LANES), 0)
    from_row = lax.broadcasted_iota(jnp.int32, (LANES, n_seq * LANES), 1)
    offset = from_row - to_row // pack * res
    copy_at = lax.broadcasted_iota(jnp.int32, (LANES, pack * ch), 1) // ch
    group_at = lax.broadcasted_iota(jnp.int32, (LANES, pack * ch), 0) % pack
    for q in range(2):
        pltpu.matmul_push_rhs(jnp.concatenate([sides] * 2, 1), 0, q)
    for part in range(n_seq):
        for i in range(res):
            q = i % 2
            pick = (offset == part * LANES + i).astype(F32).astype(BF16)
            pltpu.matmul_acc_lhs(
                row_acc[q], pick, load_staged_rhs=0 if part == 0 and i < 2 else None
            )
            block = pltpu.matmul_pop(row_acc[q])[:, : pack * ch]
            blocks[part * LANES : (part + 1) * LANES, i * pack * ch : (i + 1) * pack * ch] = (
                jnp.where(group_at == copy_at, block, 0.0).astype(BF16)
            )

    for level in range(levels):
        above = jnp.minimum((level + 1) * step - 1 - my_res, step)

        @pl.when(above > 0)
        def _():
            pl.semaphore_wait(ready_sem.at[level], above)

            def higher(n, carry):
                @pl.when(level * step + n > my_res)
                def _():
                    send_right(level * step + n).start()

                return carry

            lax.fori_loop(0, step, higher, 0, unroll=short)

    tiles = high // per_row
    wide = 2 * LANES

    def push_weights():
        for q in range(2):
            pltpu.matmul_push_rhs(blocks[:, q * wide : (q + 1) * wide], 0, q)
            pltpu.matmul_push_rhs(mixed_ref[q * wide : (q + 1) * wide, :], 1, q)

    def first_matmul(n, lhs):
        for q in range(2):
            pltpu.matmul_acc_lhs(first_acc[q][n], lhs, load_staged_rhs=None if n else 0)

    def second_matmul(n, lhs):
        for q in range(2):
            pltpu.matmul_acc_lhs(second_acc[q][n], lhs[q], load_staged_rhs=None if n else 1)

    def second_result(n):
        both = pltpu.matmul_pop(second_acc[0][n]) + pltpu.matmul_pop(second_acc[1][n])
        found = []
        for at in range(0, 2 * SUBLANES, SUBLANES):
            piece = both[at : at + res, :cz]
            for h in range(1, per_row):
                piece = piece + both[at + h * res : at + (h + 1) * res, h * cz : (h + 1) * cz]
            found.append(piece)
        return found

    def lanes_of(outer, i):
        return outer[i // 2][:, i % 2 * LANES : (i % 2 + 1) * LANES]

    def columns(n):
        pairs = range(group // 2)
        for pair in pairs:
            for tile in range(tiles):
                lhs = [
                    right_got[
                        pl.ds(part * half + n * group + 2 * pair, 2),
                        tile * SUBLANES : (tile + 1) * SUBLANES,
                    ].reshape(2 * SUBLANES, LANES)
                    for part in range(n_seq)
                ]
                first_matmul(pair * tiles + tile, jnp.concatenate(lhs, 1))
        outer = [
            [pltpu.matmul_pop(first_acc[q][k]) for q in range(2)] for k in range(len(pairs) * tiles)
        ]
        for pair in pairs:
            for i in range(res):
                lhs = [
                    jnp.concatenate(
                        [
                            lanes_of(outer[pair * tiles + 2 * q + tile], i).astype(BF16)
                            for tile in range(tiles // 2)
                        ],
                        1,
                    )
                    for q in range(2)
                ]
                second_matmul(pair * res + i, lhs)
        for pair in pairs:
            for i in range(res):
                found = second_result(pair * res + i)
                at = pl.ds(pl.multiple_of((n * group + 2 * pair) * res, SUBLANES), SUBLANES)
                held[i, at, :] = jnp.concatenate(found, 0) * inv_count + bias_ref[...]

    if half == group:
        push_weights()
        await_bytes(right_got.at[pl.ds(0, n_res - 1)], rrecv_sem.at[0])
        columns(0)
    else:
        await_bytes(right_got.at[pl.ds(0, n_res - 1)], rrecv_sem.at[0])

        @pl.loop(0, half // group)
        def _(n):
            push_weights()
            columns(n)

    push_weights()
    my_last = last_slot(my_res)
    my_part = lax.rem(n_seq - my_seq, n_seq)
    await_bytes(right_got.at[n_res], rrecv_sem.at[1])
    for pair in range(tiles // 2):
        block = right_got[n_res, pair * 2 * SUBLANES : (pair + 1) * 2 * SUBLANES, :]
        zero = jnp.zeros_like(block)
        lhs = [jnp.where(my_part == part, block, zero) for part in range(n_seq)]
        first_matmul(pair, jnp.concatenate(lhs, 1))
    outer = [[pltpu.matmul_pop(first_acc[q][k]) for q in range(2)] for k in range(tiles // 2)]
    for pair in range(res // 2):
        lhs = []
        for q in range(2):
            pieces = []
            for tile in range(tiles // 2):
                at = slice(tile * SUBLANES, (tile + 1) * SUBLANES)
                pieces.append(
                    jnp.concatenate(
                        [lanes_of(outer[q], 2 * pair + k)[at] for k in range(2)], 0
                    ).astype(BF16)
                )
            lhs.append(jnp.concatenate(pieces, 1))
        second_matmul(pair, lhs)
    found = [piece for pair in range(res // 2) for piece in second_result(pair)]

    def finish(n):
        for i in range(res):
            piece = found[i] * inv_count
            for pair in range(group // 2):
                slot = n * group + 2 * pair
                at = pl.ds(pl.multiple_of(slot * res, SUBLANES), SUBLANES)
                added = [jnp.where(my_last == slot + k, piece, 0.0) for k in range(2)]
                out_ref[i, at, :] = (held[i, at, :] + jnp.concatenate(added, 0)).astype(BF16)

    if half == group:
        finish(0)
    else:

        @pl.loop(0, half // group)
        def _(n):
            finish(n)

    for copy in left_sends:
        copy.wait_send()

    @pl.when(away == 0)
    def _():
        await_bytes(right_got.at[pl.ds(0, n_res - 1)], load_sem.at[0])

    @pl.when(away != 0)
    def _():
        await_bytes(right_got.at[pl.ds(0, n_res)], load_sem.at[0])


def scoped(n_res, n_seq, *refs):
    accumulators = [
        pltpu.ACC(q)((m, 2 * LANES), F32) for q in range(2) for m in [32, LANES] + [16] * 16
    ]
    pl.run_scoped(
        functools.partial(kernel, n_res, n_seq, *refs),
        pltpu.SemaphoreType.DMA((n_seq + 1,)),
        pltpu.SemaphoreType.DMA((n_seq - 1,)),
        pltpu.SemaphoreType.DMA((2,)),
        pltpu.SemaphoreType.REGULAR((2 * n_seq,)),
        *accumulators,
    )


def on_device(alignment, ln_gain, proj_left, proj_right, out_weight, out_bias):
    n_res, n_seq = lax.axis_size("res"), lax.axis_size("seq")
    seqs, res, width = alignment.shape
    ch = proj_left.shape[1]
    cz = out_weight.shape[1]
    half = n_res // n_seq
    cols = res * half
    pack = LANES // seqs
    rows = res * (ch // pack)
    wide = res * pack * ch
    group = math.gcd(half, 4)
    per_row = SUBLANES // res
    unit = 2 * LANES * 4
    early = (seqs * res * width + ch * width) * 2 + width * 4
    late = ch * ch * cz * 2 + cz * 4
    return pl.pallas_call(
        functools.partial(scoped, n_res, n_seq),
        out_shape=pltpu.VMEM((res, cols, cz), BF16),
        in_specs=[pl.BlockSpec(memory_space=pl.ANY)] * 6,
        out_specs=pl.BlockSpec(memory_space=pltpu.VMEM),
        scratch_shapes=[
            pltpu.VMEM((seqs, res, width), BF16),
            pltpu.VMEM((1, width), F32),
            pltpu.VMEM((ch, width), BF16),
            pltpu.VMEM((ch, width), BF16),
            pltpu.VMEM((ch * ch, cz), BF16),
            pltpu.VMEM((1, cz), F32),
            pltpu.VMEM((ch * ch, cz), F32),
            pltpu.VMEM((ch * ch // per_row, per_row * cz), BF16),
            pltpu.VMEM((res * seqs, pack * ch), BF16),
            pltpu.VMEM((n_seq - 1, res * seqs, pack * ch), BF16),
            pltpu.VMEM((n_seq * LANES, wide), BF16),
            pltpu.VMEM((rows, LANES), BF16),
            pltpu.VMEM((n_res + 1, rows, LANES), BF16),
            pltpu.VMEM((rows, LANES), F32),
            pltpu.VMEM((res, cols, cz), F32),
            pltpu.VMEM((early // unit, 2, LANES), F32),
            pltpu.VMEM((late // (unit // 2), 1, LANES), F32),
        ],
        compiler_params=pltpu.CompilerParams(collective_id=0, has_side_effects=True),
    )(
        alignment,
        ln_gain.reshape(1, width),
        proj_left.T,
        proj_right.T,
        out_weight,
        out_bias.reshape(1, cz),
    )


def solution(mesh):
    placed = (P(("groups", "seq"), "res", None), P(), P(), P(), P(), P())
    return jax.shard_map(
        on_device,
        mesh=mesh,
        in_specs=placed,
        out_specs=P(("groups", "res"), "seq", None),
        check_vma=False,
    )
```
